32 devices in a mesh: px: 8 (over z, x), py: 4 (over y, core).
Axes of the slice: x: 2, y: 2, z: 4, core: 2. Of those that a mesh axis runs over, the one named last changes fastest.
Arguments:
- potential: float32 [256, 256, 256], P(('px', 'py')), may hold values from 0 to 1
- recovery: float32 [256, 256, 256], P(('px', 'py')), may hold values from 0 to 2
- stimulus: float32 [256, 256, 256], P(('px', 'py')), may hold values from -8 to 8
- conductivity: float32 [256, 256, 256], P('px', 'py'), may hold values from 0.2 to 5
Outputs:
- potential_next: float32 [256, 256, 256], P(('px', 'py'))
- recovery_next: float32 [256, 256, 256], P(('px', 'py'))
The draws below stay inside these ranges and needn't reach their ends.
All inputs are finite; a program needn't handle non-finite values.
Results may differ from the reference program's by a relative error of at most 0.0003.
Values sent between devices are 32-bit elements; how exact they have to be, the bound alone decides.
No kernel may reach another device: no remote copies, remote signals or barrier semaphores. Data moves between devices by JAX's collectives and lax.ppermute only.
A program may use at most 128 MiB of HBM per device.

```python
import math
import jax
import jax.numpy as jnp

GX = 256
GY = 256
GZ = 256
ITERS = 4


def draw_stimulus(key, part):
    noise = jnp.clip(jax.random.normal(key, (GX, GY, GZ), jnp.float32), -4.0, 4.0) * 2.0
    return noise


def block_scale(rng, shape, split, low, high):
    level, own = 1.0, jax.random.fold_in(rng, 6)
    for axis_at, parts in split:
        heights = jnp.exp(jax.random.uniform(jax.random.fold_in(own, axis_at), (parts,), jnp.float32, low / len(split), high / len(split)))
        level = level * jnp.repeat(heights, shape[axis_at] // parts).reshape([-1 if axis == axis_at else 1 for axis in range(len(shape))])
    return level


def setup_inputs(seed: int = 0) -> dict:
    key_list = jax.random.split(jax.random.key(seed), 5)
    potential = jnp.clip(1.0 * jax.random.uniform(key_list[0], (GX, GY, GZ), jnp.float32) ** block_scale(key_list[0], (GX, GY, GZ), ((0, 32),), -0.2, 0.2), 0.0, 1.0)
    recovery = jnp.clip(2.0 * jax.random.uniform(key_list[1], (GX, GY, GZ), jnp.float32) ** block_scale(key_list[1], (GX, GY, GZ), ((0, 32),), -0.2, 0.2), 0.0, 2.0)
    stimulus = draw_stimulus(jax.random.fold_in(key_list[4], 71), 0)
    conductivity = jnp.clip(jnp.exp(math.log(5.0) - 3.218876 * jax.random.uniform(key_list[3], (GX, GY, GZ), jnp.float32) ** block_scale(key_list[3], (GX, GY, GZ), ((0, 8), (1, 4)), -0.2, 0.2)), 0.2, 5.0)
    return dict(potential=potential, recovery=recovery, stimulus=stimulus, conductivity=conductivity)


mass_rate = 0.01
mean_conduct = 1.0
excite_gain = 8.0
threshold = 0.15
base_rate = 0.002
rate_slope = 0.2
rate_shift = 0.3
time_step = 0.1


def face_conductance(conductivity):
    result_list = []
    for dimension in range(3):
        for offset in (-1, 1):
            result_list.append(0.5 * (conductivity + jnp.roll(conductivity, offset, dimension)))
    return result_list


def operate(field, conductance):
    result_sum = mass_rate * field
    position = 0
    for dimension in range(3):
        for offset in (-1, 1):
            result_sum = result_sum + conductance[position] * (field - jnp.roll(field, offset, dimension))
            position = position + 1
    return result_sum


def wave_term(length):
    modes = jnp.arange(length, dtype=jnp.int32).astype(jnp.float32)
    return 2.0 - 2.0 * jnp.cos((2.0 * math.pi / length) * modes)


def precondition(residual, symbol):
    spectrum = jnp.fft.fftn(residual)
    return jnp.real(jnp.fft.ifftn(spectrum / symbol)).astype(residual.dtype)


def reference(potential, recovery, stimulus, conductivity):
    drive = excite_gain * potential * (potential - threshold) * (1.0 - potential) - potential * recovery
    v_star = potential + time_step * (drive + stimulus)
    rate = base_rate + rate_slope * recovery / (potential + rate_shift)
    recovery_next = recovery + time_step * rate * (-recovery - excite_gain * potential * (potential - threshold - 1.0))
    conductance = face_conductance(conductivity)
    symbol = mass_rate + mean_conduct * (wave_term(GX)[:, None, None] + wave_term(GY)[None, :, None] + wave_term(GZ)[None, None, :])
    solution = v_star
    residual = mass_rate * v_star - operate(solution, conductance)
    precond = precondition(residual, symbol)
    direction = precond
    product_now = jnp.sum(residual * precond)
    for step in range(ITERS):
        image = operate(direction, conductance)
        alpha = product_now / jnp.sum(direction * image)
        solution = solution + alpha * direction
        residual = residual - alpha * image
        if step < ITERS - 1:
            precond = precondition(residual, symbol)
            product_next = jnp.sum(residual * precond)
            direction = precond + (product_next / product_now) * direction
            product_now = product_next
    return solution, recovery_next
```

```python
import functools
import math

import jax
import jax.numpy as jnp
import numpy as np
from jax import lax
from jax.experimental import pallas as pl
from jax.experimental.pallas import tpu as pltpu
from jax.sharding import PartitionSpec as P

ITERS = 4
mass_rate = 0.01
mean_conduct = 1.0
excite_gain = 8.0
threshold = 0.15
base_rate = 0.002
rate_slope = 0.2
rate_shift = 0.3
time_step = 0.1
alpha_low = 0.199
alpha_high = 5.03

AXES = ("px", "py")
SUB = 8
LANE = 128
VMEM = pltpu.MemorySpace.VMEM


def cas_parts(length):
    steps = np.arange(length)
    angle = 2.0 * np.pi / length * (steps[:, None] * steps[None, :] % length)
    table = np.cos(angle) + np.sin(angle)
    high = table.astype(jnp.bfloat16)
    low = (table - high.astype(np.float64)).astype(jnp.bfloat16)
    return high, low


def wave_term(length):
    return 2.0 - 2.0 * np.cos(2.0 * np.pi / length * np.arange(length))


def mode_tables(gx, gy, gz, planes):
    sigma = mass_rate / mean_conduct + wave_term(gy)[:, None] + wave_term(gz)[None, :]
    rho = 1.0 / (1.0 + 0.5 * sigma + np.sqrt(sigma + 0.25 * sigma * sigma))
    scale = rho / (1.0 - rho * rho) / (mean_conduct * gy * gz)
    block = rho**planes
    closure = 1.0 / (1.0 - rho**gx)
    return rho, scale, block, closure


def split_bf16(x):
    high = x.astype(jnp.bfloat16)
    low = (x - high.astype(jnp.float32)).astype(jnp.bfloat16)
    return high, low


def dot(a, b):
    return jnp.dot(a, b, preferred_element_type=jnp.float32)


def right_transform(xh, xl, hh, hl):
    return dot(xh, hh) + dot(xl, hh) + dot(xh, hl)


def left_transform(xh, xl, hh, hl):
    return dot(hh, xh) + dot(hh, xl) + dot(hl, xh)


class Shape:
    def __init__(self, planes, gy, gz, devices):
        self.planes, self.gy, self.gz, self.devices = planes, gy, gz, devices
        self.gx = planes * devices
        self.halves = gz // LANE
        self.per_group = 2 * self.halves
        self.slots = gy // SUB * self.per_group // devices
        assert self.per_group % self.slots == 0
        self.rows = self.slots * SUB

    def place(self, group, kind, half):
        q = kind * self.halves + half
        return group * (self.per_group // self.slots) + q // self.slots, q % self.slots * SUB


def emit_forward(sh, source, rho, hh_ref, hl_ref, f_ref, pay_ref, scal):
    hh = hh_ref[...]
    hl = hl_ref[...]

    def plane(j, _):
        xh, xl = split_bf16(source(j))
        th, tl = split_bf16(right_transform(xh, xl, hh, hl))
        f_ref[j] = left_transform(th, tl, hh, hl)
        return 0

    lax.fori_loop(0, sh.planes, plane, 0)

    def group(g, _):
        row = pl.multiple_of(g * SUB, SUB)
        for half in range(sh.halves):
            lanes = slice(half * LANE, (half + 1) * LANE)
            decay = rho[pl.ds(row, SUB), lanes]
            f = [f_ref[j, pl.ds(row, SUB), lanes] for j in range(sh.planes)]
            p = f[0]
            e = f[-1]
            for j in range(1, sh.planes):
                p = f[j] + decay * p
                e = f[sh.planes - 1 - j] + decay * e
            for kind, value in ((0, p), (1, e)):
                d, at = sh.place(g, kind, half)
                pay_ref[d, pl.ds(at, SUB), :] = value
        return 0

    lax.fori_loop(0, sh.gy // SUB, group, 0)

    def spread(d, _):
        pay_ref[d, pl.ds(sh.rows, SUB), :] = scal
        return 0

    lax.fori_loop(0, sh.devices, spread, 0)


def stencil(sh, j, here, before, after, gx_ref, gy_ref, gz_ref):
    acc = gx_ref[j + 1] * (here - after) - gx_ref[j] * (before - here)
    flux = gy_ref[j] * (here - pltpu.roll(here, sh.gy - 1, 0))
    acc = acc + flux - pltpu.roll(flux, 1, 0)
    flux = gz_ref[j] * (here - pltpu.roll(here, sh.gz - 1, 1))
    return acc + flux - pltpu.roll(flux, 1, 1)


def fold(sh, x):
    return jnp.sum(x.reshape(sh.gy // SUB, SUB, sh.gz), axis=0)


def scal_tile(sh, parts):
    rows = []
    for part in parts:
        row = jnp.sum(part, axis=0, keepdims=True)
        total = row[:, :LANE]
        for half in range(1, sh.halves):
            total = total + row[:, half * LANE : (half + 1) * LANE]
        rows.append(total)
    rows.append(jnp.zeros((SUB - len(rows), LANE), jnp.float32))
    return jnp.concatenate(rows, axis=0)


def start_kernel(
    sh, parts, u, ulo, uhi, craw, clo, chi, rho, hh, hl, gx, gy, gz, r, f, pay, c
):
    wide = sh.gy // parts
    for k in range(parts):
        c[:, k * wide : (k + 1) * wide, :] = 0.5 * craw[k]

    def faces(j, _):
        own = c[j]
        gy[j] = own + pltpu.roll(own, sh.gy - 1, 0)
        gz[j] = own + pltpu.roll(own, sh.gz - 1, 1)
        return 0

    lax.fori_loop(0, sh.planes, faces, 0)
    gx[0] = 0.5 * clo[0] + c[0]
    gx[sh.planes] = 0.5 * chi[0] + c[sh.planes - 1]

    def cross(j, _):
        gx[j] = c[j - 1] + c[j]
        return 0

    lax.fori_loop(1, sh.planes, cross, 0)

    last = sh.planes - 1
    r[0] = -stencil(sh, 0, u[0], ulo[0], u[1], gx, gy, gz)

    def inner(j, _):
        r[j] = -stencil(sh, j, u[j], u[j - 1], u[j + 1], gx, gy, gz)
        return 0

    lax.fori_loop(1, last, inner, 0)
    r[last] = -stencil(sh, last, u[last], u[last - 1], uhi[0], gx, gy, gz)
    emit_forward(
        sh, lambda j: r[j], rho, hh, hl, f, pay, jnp.zeros((SUB, LANE), jnp.float32)
    )


def scan_kernel(sh, first, *refs):
    recv, decay, closure, onward = refs[:4]
    if first:
        (out,) = refs[4:]
    else:
        coef, out, coef_out = refs[4:]
    count = sh.devices

    def run(rows, forward, store):
        a = decay[rows]
        order = (lambda i: i) if forward else (lambda i: count - 1 - i)

        def total(i, s):
            return recv[order(i), rows, :] + a * s

        zero = jnp.zeros(a.shape, jnp.float32)
        carry = lax.fori_loop(0, count, total, zero, unroll=8) * closure[rows]

        def step(i, carry):
            store(order(i), carry)
            return recv[order(i), rows, :] + a * carry

        lax.fori_loop(0, count, step, carry, unroll=8)

    if sh.slots == sh.per_group:
        half = sh.rows // 2
        for rows, forward in ((slice(0, half), True), (slice(half, sh.rows), False)):

            def store(d, x, rows=rows):
                out[d, rows, :] = x

            run(rows, forward, store)
    else:
        rows = slice(0, sh.rows)
        take = onward[...]

        def store_forward(d, x):
            out[d] = x

        def store_backward(d, x):
            out[d] = jnp.where(take > 0.5, out[d], x)

        run(rows, True, store_forward)
        run(rows, False, store_backward)

    if not first:
        sums = sum_rows(sh.devices, recv, sh.rows)
        coef_out[...] = next_coefficients(sums, coef[...], sh.gz)


def sum_rows(count, recv, at):
    def add(d, s):
        return s + recv[d, at : at + SUB, :]

    return lax.fori_loop(1, count, add, recv[0, at : at + SUB, :], unroll=4)


def next_coefficients(sums, previous, width):
    product = jnp.maximum(jnp.sum(sums[0:1], axis=1, keepdims=True), 0.0)
    curve = jnp.sum(sums[1:2], axis=1, keepdims=True)
    product = jnp.broadcast_to(product, (1, width))
    curve = jnp.broadcast_to(curve, (1, width))
    old_product = previous[0:1]
    old_alpha = previous[1:2]
    started = old_product > 0.0
    beta = jnp.where(started, product / jnp.where(started, old_product, 1.0), 0.0)
    curve = curve - beta * product / jnp.where(old_alpha > 0.0, old_alpha, 1.0)
    usable = curve > 0.0
    alpha = jnp.where(usable, product / jnp.where(usable, curve, 1.0), alpha_low)
    alpha = jnp.clip(alpha, alpha_low, alpha_high)
    return jnp.concatenate(
        [product, alpha, beta, jnp.zeros((SUB - 3, width), jnp.float32)], axis=0
    )


def emit_inverse(sh, f, carry, rho, scale, hh_ref, hl_ref, uh, ul, m):
    tall = 2 * SUB

    def group(i, _):
        row = pl.multiple_of(i * tall, tall)
        for half in range(sh.halves):
            lanes = slice(half * LANE, (half + 1) * LANE)
            decay = rho[pl.ds(row, tall), lanes]
            gain = scale[pl.ds(row, tall), lanes]
            ends = []
            for kind in range(2):
                tiles = []
                for g in (2 * i, 2 * i + 1):
                    d, at = sh.place(g, kind, half)
                    tiles.append(carry[d, pl.ds(at, SUB), :])
                ends.append(jnp.concatenate(tiles, axis=0))
            first, final = ends

            def put(j, value):
                high, low = split_bf16(gain * value)
                uh[j, pl.ds(row, tall), lanes] = high
                ul[j, pl.ds(row, tall), lanes] = low

            fields = [f[j, pl.ds(row, tall), lanes] for j in range(sh.planes)]
            back = [None] * sh.planes
            e = final
            for j in reversed(range(sh.planes)):
                back[j] = decay * e
                e = fields[j] + back[j]
            put(0, first + decay * e)
            p = first
            for j in range(sh.planes):
                p = fields[j] + decay * p
                put(j + 1, p + back[j])
            put(sh.planes + 1, decay * p + final)
        return 0

    lax.fori_loop(0, sh.gy // tall, group, 0)
    hh = hh_ref[...]
    hl = hl_ref[...]

    def plane(j, _):
        th, tl = split_bf16(right_transform(uh[j], ul[j], hh, hl))
        m[j] = left_transform(th, tl, hh, hl)
        return 0

    lax.fori_loop(0, sh.planes + 2, plane, 0)


def step_kernel(sh, stage, *refs):
    names = ["f", "carry", "rho", "scale", "hh", "hl", "gx", "gy", "gz", "r"]
    if stage > 0:
        names += ["coef", "z", "w"]
    if stage > 1:
        names += ["s", "q", "t"]
    last = stage == ITERS - 1
    if stage == 0:
        outs = ["z_new", "w_new"]
    elif last:
        outs = ["z_new"]
    else:
        outs = ["z_new", "w_new", "r_new", "s_new", "q_new", "t_new"]
        if stage == 1:
            outs.remove("s_new")
    outs += ["pay"] if last else ["f_new", "pay"]
    scratch = ["uh", "ul", "m"]
    if last:
        scratch += []
    k = dict(zip(names + outs + scratch, refs, strict=True))
    m = k["m"]
    emit_inverse(sh, k["f"], k["carry"], k["rho"], k["scale"], k["hh"], k["hl"], k["uh"], k["ul"], m)
    if stage > 0:
        alpha = k["coef"][1:2, :]
        beta = k["coef"][2:3, :]

    def plane(j, sums):
        here = m[j + 1]
        image = mass_rate * here + mean_conduct * stencil(
            sh, j, here, m[j], m[j + 2], k["gx"], k["gy"], k["gz"]
        )
        if stage == 0:
            z, w, r = here, image, k["r"][j]
        else:
            s, q, t = k["w"][j], here, image
            if stage > 1:
                s = s + beta * k["s"][j]
                q = q + beta * k["q"][j]
                t = t + beta * k["t"][j]
            r = k["r"][j] - alpha * s
            z = k["z"][j] - alpha * q
            w = k["w"][j] - alpha * t
            if not last:
                k["r_new"][j] = r
                k["q_new"][j] = q
                k["t_new"][j] = t
                if stage > 1:
                    k["s_new"][j] = s
        k["z_new"][j] = z
        if not last:
            k["w_new"][j] = w
        return (sums[0] + fold(sh, r * z), sums[1] + fold(sh, w * z))

    zero = jnp.zeros((SUB, sh.gz), jnp.float32)
    scal = scal_tile(sh, lax.fori_loop(0, sh.planes, plane, (zero, zero)))
    if last:
        pay = k["pay"]

        def spread(d, _):
            pay[d] = scal
            return 0

        lax.fori_loop(0, sh.devices, spread, 0)
    else:
        w_new = k["w_new"]
        emit_forward(sh, lambda j: w_new[j], k["rho"], k["hh"], k["hl"], k["f_new"], k["pay"], scal)


def finish_kernel(sh, *refs):
    coefs = refs[: ITERS - 1]
    recv = refs[ITERS - 1]
    u = refs[ITERS]
    fields = refs[ITERS + 1 : 2 * ITERS + 1]
    out = refs[-1]
    rows = [c[...] for c in coefs]
    rows.append(next_coefficients(sum_rows(sh.devices, recv, 0), rows[-1], sh.gz))
    weight = rows[-1][1:2]
    weights = [weight]
    for i in reversed(range(ITERS - 1)):
        weight = rows[i][1:2] + rows[i + 1][2:3] * weight
        weights.insert(0, weight)

    def plane(j, _):
        total = u[j]
        for weight, field in zip(weights, fields):
            total = total + weight * field[j]
        out[j] = total
        return 0

    lax.fori_loop(0, sh.planes, plane, 0)


def call(kernel, name, out_shapes, operands, scratch=(), aliases=None):
    whole = pl.BlockSpec(memory_space=VMEM)
    return pl.pallas_call(
        kernel,
        name=name,
        out_shape=[jax.ShapeDtypeStruct(s, jnp.float32) for s in out_shapes],
        in_specs=[whole] * len(operands),
        out_specs=[whole] * len(out_shapes),
        scratch_shapes=list(scratch),
        input_output_aliases=aliases or {},
        compiler_params=pltpu.CompilerParams(vmem_limit_bytes=60 * 1024 * 1024),
    )(*operands)


def exchange(x):
    return lax.all_to_all(x, AXES, split_axis=0, concat_axis=0, tiled=True)


def neighbours(first, final, axes):
    count = lax.axis_size(axes)
    return (
        lax.ppermute(final, axes, [(i, (i + 1) % count) for i in range(count)]),
        lax.ppermute(first, axes, [((i + 1) % count, i) for i in range(count)]),
    )


def local(potential, recovery, stimulus, conductivity):
    parts = lax.axis_size("py")
    devices = lax.axis_size("px") * parts
    planes, gy, gz = potential.shape
    sh = Shape(planes, gy, gz, devices)

    wide = conductivity.shape[1]
    craw = lax.all_to_all(
        conductivity.reshape(parts, planes, wide, gz), "py", split_axis=0, concat_axis=0, tiled=True
    )
    drive = (
        excite_gain * potential * (potential - threshold) * (1.0 - potential) - potential * recovery
    )
    v_star = potential + time_step * (drive + stimulus)
    rate = base_rate + rate_slope * recovery / (potential + rate_shift)
    recovery_next = recovery + time_step * rate * (
        -recovery - excite_gain * potential * (potential - threshold - 1.0)
    )
    ulo, uhi = neighbours(v_star[:1], v_star[-1:], AXES)

    def edge(j):
        return craw[:, j].reshape(1, gy, gz)

    clo, chi = neighbours(edge(0), edge(planes - 1), AXES)

    rho, scale, block, closure = mode_tables(sh.gx, gy, gz, planes)
    groups = gy // SUB

    def own_tiles(table):
        tiles = table.astype(np.float32).reshape(groups, SUB, sh.halves, LANE).transpose(0, 2, 1, 3)
        both = np.concatenate([tiles, tiles], axis=1).reshape(devices, sh.rows, LANE)
        return lax.dynamic_index_in_dim(jnp.asarray(both), lax.axis_index(AXES), 0, False)

    block = own_tiles(block)
    closure = own_tiles(closure)
    slot = lax.axis_index(AXES) * sh.slots + jnp.arange(sh.rows, dtype=jnp.int32)[:, None] // SUB
    onward = jnp.broadcast_to(
        (slot % sh.per_group < sh.halves).astype(jnp.float32), (sh.rows, LANE)
    )
    rho = jnp.asarray(rho.astype(np.float32))
    scale = jnp.asarray(scale.astype(np.float32))
    hh, hl = (jnp.asarray(x) for x in cas_parts(gy))

    slab = (planes, gy, gz)
    payload = (devices, sh.rows + SUB, LANE)
    carries = (devices, sh.rows, LANE)
    tables = [rho, hh, hl]
    gxf, gyf, gzf, r, f, pay = call(
        functools.partial(start_kernel, sh, parts),
        "start",
        [(planes + 1, gy, gz), slab, slab, slab, slab, payload],
        [v_star, ulo, uhi, craw, clo, chi] + tables,
        [pltpu.VMEM(slab, jnp.float32)],
    )
    spectral = [
        pltpu.VMEM((planes + 2, gy, gz), jnp.bfloat16),
        pltpu.VMEM((planes + 2, gy, gz), jnp.bfloat16),
        pltpu.VMEM((planes + 2, gy, gz), jnp.float32),
    ]
    coef = jnp.zeros((SUB, gz), jnp.float32)
    coefs = []
    basis = []
    z = w = s = q = t = None
    for stage in range(ITERS):
        recv = exchange(pay)
        if stage == 0:
            (carry,) = call(
                functools.partial(scan_kernel, sh, True),
                "scan0",
                [carries],
                [recv, block, closure, onward],
            )
        else:
            carry, coef = call(
                functools.partial(scan_kernel, sh, False),
                f"scan{stage}",
                [carries, (SUB, gz)],
                [recv, block, closure, onward, coef],
            )
            coefs.append(coef)
        carry = exchange(carry)
        operands = [f, carry, rho, scale, hh, hl, gxf, gyf, gzf, r]
        if stage > 0:
            operands += [coef, z, w]
        if stage > 1:
            operands += [s, q, t]
        kernel = functools.partial(step_kernel, sh, stage)
        if stage == 0:
            z, w, f, pay = call(kernel, "step0", [slab, slab, slab, payload], operands, spectral)
        elif stage < ITERS - 1:
            shapes = [slab] * (5 if stage == 1 else 6) + [slab, payload]
            old_w = w
            results = call(kernel, f"step{stage}", shapes, operands, spectral)
            if stage == 1:
                z, w, r, q, t, f, pay = results
                s = old_w
            else:
                z, w, r, s, q, t, f, pay = results
        else:
            z, pay = call(kernel, f"step{stage}", [slab, (devices, SUB, LANE)], operands, spectral)
        basis.append(z)
    recv = exchange(pay)
    (potential_next,) = call(
        functools.partial(finish_kernel, sh), "finish", [slab], coefs + [recv, v_star] + basis
    )
    return potential_next, recovery_next


def solution(mesh):
    in_specs = (
        P(AXES, None, None),
        P(AXES, None, None),
        P(AXES, None, None),
        P("px", "py", None),
    )
    out_specs = (P(AXES, None, None), P(AXES, None, None))
    return jax.shard_map(local, mesh=mesh, in_specs=in_specs, out_specs=out_specs, check_vma=False)
```

```python
import functools
import math

import jax
import jax.numpy as jnp
import numpy as np
from jax import lax
from jax.experimental import pallas as pl
from jax.experimental.pallas import tpu as pltpu
from jax.sharding import PartitionSpec as P

ITERS = 4
mass_rate = 0.01
mean_conduct = 1.0
excite_gain = 8.0
threshold = 0.15
base_rate = 0.002
rate_slope = 0.2
rate_shift = 0.3
time_step = 0.1
alpha_low = 0.199
alpha_high = 5.03

AXES = ("px", "py")
SUB = 8
LANE = 128
VMEM = pltpu.MemorySpace.VMEM


def cas_parts(length):
    steps = np.arange(length)
    angle = 2.0 * np.pi / length * (steps[:, None] * steps[None, :] % length)
    table = np.cos(angle) + np.sin(angle)
    high = table.astype(jnp.bfloat16)
    low = (table - high.astype(np.float64)).astype(jnp.bfloat16)
    return high, low


def wave_term(length):
    return 2.0 - 2.0 * np.cos(2.0 * np.pi / length * np.arange(length))


def mode_tables(gx, gy, gz, planes):
    sigma = mass_rate / mean_conduct + wave_term(gy)[:, None] + wave_term(gz)[None, :]
    rho = 1.0 / (1.0 + 0.5 * sigma + np.sqrt(sigma + 0.25 * sigma * sigma))
    scale = rho / (1.0 - rho * rho) / (mean_conduct * gy * gz)
    block = rho**planes
    closure = 1.0 / (1.0 - rho**gx)
    return rho, scale, block, closure


def split_bf16(x):
    high = x.astype(jnp.bfloat16)
    low = (x - high.astype(jnp.float32)).astype(jnp.bfloat16)
    return high, low


def dot(a, b):
    return jnp.dot(a, b, preferred_element_type=jnp.float32)


def right_transform(xh, xl, hh, hl):
    return dot(xh, hh) + dot(xl, hh) + dot(xh, hl)


def left_transform(xh, xl, hh, hl):
    return dot(hh, xh) + dot(hh, xl) + dot(hl, xh)


def together(count):
    return max(k for k in range(1, 6) if count % k == 0)


class Shape:
    def __init__(self, planes, gy, gz, devices):
        self.planes, self.gy, self.gz, self.devices = planes, gy, gz, devices
        self.gx = planes * devices
        self.halves = gz // LANE
        self.per_group = 2 * self.halves
        self.slots = gy // SUB * self.per_group // devices
        assert self.per_group % self.slots == 0
        self.rows = self.slots * SUB

    def place(self, group, kind, half):
        q = kind * self.halves + half
        return group * (self.per_group // self.slots) + q // self.slots, q % self.slots * SUB


def emit_forward(sh, source, rho, hh_ref, hl_ref, f_ref, pay_ref, scal):
    hh = hh_ref[...]
    hl = hl_ref[...]

    many = together(sh.planes)

    def pair(i, _):
        js = [i * many + k for k in range(many)]
        src = [split_bf16(source(j)) for j in js]
        right = [right_transform(xh, xl, hh, hl) for xh, xl in src]
        parts = [split_bf16(x) for x in right]
        for j, (th, tl) in zip(js, parts):
            f_ref[j] = left_transform(th, tl, hh, hl)
        return 0

    lax.fori_loop(0, sh.planes // many, pair, 0)

    def group(g, _):
        row = pl.multiple_of(g * SUB, SUB)
        for half in range(sh.halves):
            lanes = slice(half * LANE, (half + 1) * LANE)
            decay = rho[pl.ds(row, SUB), lanes]
            f = [f_ref[j, pl.ds(row, SUB), lanes] for j in range(sh.planes)]
            p = f[0]
            e = f[-1]
            for j in range(1, sh.planes):
                p = f[j] + decay * p
                e = f[sh.planes - 1 - j] + decay * e
            for kind, value in ((0, p), (1, e)):
                d, at = sh.place(g, kind, half)
                pay_ref[d, pl.ds(at, SUB), :] = value
        return 0

    lax.fori_loop(0, sh.gy // SUB, group, 0)

    def spread(d, _):
        pay_ref[d, pl.ds(sh.rows, SUB), :] = scal
        return 0

    lax.fori_loop(0, sh.devices, spread, 0)


def stencil(sh, j, here, before, after, gx_ref, gy_ref, gz_ref):
    acc = gx_ref[j + 1] * (here - after) - gx_ref[j] * (before - here)
    flux = gy_ref[j] * (here - pltpu.roll(here, sh.gy - 1, 0))
    acc = acc + flux - pltpu.roll(flux, 1, 0)
    flux = gz_ref[j] * (here - pltpu.roll(here, sh.gz - 1, 1))
    return acc + flux - pltpu.roll(flux, 1, 1)


def fold(sh, x):
    return jnp.sum(x.reshape(sh.gy // SUB, SUB, sh.gz), axis=0)


def scal_tile(sh, parts):
    rows = []
    for part in parts:
        row = jnp.sum(part, axis=0, keepdims=True)
        total = row[:, :LANE]
        for half in range(1, sh.halves):
            total = total + row[:, half * LANE : (half + 1) * LANE]
        rows.append(total)
    rows.append(jnp.zeros((SUB - len(rows), LANE), jnp.float32))
    return jnp.concatenate(rows, axis=0)


def start_kernel(
    sh, parts, u, ulo, uhi, craw, clo, chi, rho, hh, hl, gx, gy, gz, r, f, pay, c
):
    wide = sh.gy // parts
    for k in range(parts):
        c[:, k * wide : (k + 1) * wide, :] = 0.5 * craw[k]

    def faces(j, _):
        own = c[j]
        gy[j] = own + pltpu.roll(own, sh.gy - 1, 0)
        gz[j] = own + pltpu.roll(own, sh.gz - 1, 1)
        return 0

    lax.fori_loop(0, sh.planes, faces, 0)
    gx[0] = 0.5 * clo[0] + c[0]
    gx[sh.planes] = 0.5 * chi[0] + c[sh.planes - 1]

    def cross(j, _):
        gx[j] = c[j - 1] + c[j]
        return 0

    lax.fori_loop(1, sh.planes, cross, 0)

    last = sh.planes - 1
    r[0] = -stencil(sh, 0, u[0], ulo[0], u[1], gx, gy, gz)

    def inner(j, _):
        r[j] = -stencil(sh, j, u[j], u[j - 1], u[j + 1], gx, gy, gz)
        return 0

    lax.fori_loop(1, last, inner, 0)
    r[last] = -stencil(sh, last, u[last], u[last - 1], uhi[0], gx, gy, gz)
    emit_forward(
        sh, lambda j: r[j], rho, hh, hl, f, pay, jnp.zeros((SUB, LANE), jnp.float32)
    )


def scan_kernel(sh, first, *refs):
    recv, decay, closure, onward = refs[:4]
    if first:
        (out,) = refs[4:]
    else:
        coef, out, coef_out = refs[4:]
    count = sh.devices

    def run(rows, forward, store):
        a = decay[rows]
        order = (lambda i: i) if forward else (lambda i: count - 1 - i)

        def total(i, s):
            return recv[order(i), rows, :] + a * s

        zero = jnp.zeros(a.shape, jnp.float32)
        carry = lax.fori_loop(0, count, total, zero, unroll=8) * closure[rows]

        def step(i, carry):
            store(order(i), carry)
            return recv[order(i), rows, :] + a * carry

        lax.fori_loop(0, count, step, carry, unroll=8)

    if sh.slots == sh.per_group:
        half = sh.rows // 2
        for rows, forward in ((slice(0, half), True), (slice(half, sh.rows), False)):

            def store(d, x, rows=rows):
                out[d, rows, :] = x

            run(rows, forward, store)
    else:
        rows = slice(0, sh.rows)
        take = onward[...]

        def store_forward(d, x):
            out[d] = x

        def store_backward(d, x):
            out[d] = jnp.where(take > 0.5, out[d], x)

        run(rows, True, store_forward)
        run(rows, False, store_backward)

    if not first:
        sums = sum_rows(sh.devices, recv, sh.rows)
        coef_out[...] = next_coefficients(sums, coef[...], sh.gz)


def sum_rows(count, recv, at):
    def add(d, s):
        return s + recv[d, at : at + SUB, :]

    return lax.fori_loop(1, count, add, recv[0, at : at + SUB, :], unroll=4)


def next_coefficients(sums, previous, width):
    product = jnp.maximum(jnp.sum(sums[0:1], axis=1, keepdims=True), 0.0)
    curve = jnp.sum(sums[1:2], axis=1, keepdims=True)
    product = jnp.broadcast_to(product, (1, width))
    curve = jnp.broadcast_to(curve, (1, width))
    old_product = previous[0:1]
    old_alpha = previous[1:2]
    started = old_product > 0.0
    beta = jnp.where(started, product / jnp.where(started, old_product, 1.0), 0.0)
    curve = curve - beta * product / jnp.where(old_alpha > 0.0, old_alpha, 1.0)
    usable = curve > 0.0
    alpha = jnp.where(usable, product / jnp.where(usable, curve, 1.0), alpha_low)
    alpha = jnp.clip(alpha, alpha_low, alpha_high)
    return jnp.concatenate(
        [product, alpha, beta, jnp.zeros((SUB - 3, width), jnp.float32)], axis=0
    )


def emit_inverse(sh, f, carry, rho, scale, hh_ref, hl_ref, uh, ul, m):
    tall = 2 * SUB

    def group(i, _):
        row = pl.multiple_of(i * tall, tall)
        for half in range(sh.halves):
            lanes = slice(half * LANE, (half + 1) * LANE)
            decay = rho[pl.ds(row, tall), lanes]
            gain = scale[pl.ds(row, tall), lanes]
            ends = []
            for kind in range(2):
                tiles = []
                for g in (2 * i, 2 * i + 1):
                    d, at = sh.place(g, kind, half)
                    tiles.append(carry[d, pl.ds(at, SUB), :])
                ends.append(jnp.concatenate(tiles, axis=0))
            first, final = ends

            def put(j, value):
                high, low = split_bf16(gain * value)
                uh[j, pl.ds(row, tall), lanes] = high
                ul[j, pl.ds(row, tall), lanes] = low

            fields = [f[j, pl.ds(row, tall), lanes] for j in range(sh.planes)]
            back = [None] * sh.planes
            e = final
            for j in reversed(range(sh.planes)):
                back[j] = decay * e
                e = fields[j] + back[j]
            put(0, first + decay * e)
            p = first
            for j in range(sh.planes):
                p = fields[j] + decay * p
                put(j + 1, p + back[j])
            put(sh.planes + 1, decay * p + final)
        return 0

    lax.fori_loop(0, sh.gy // tall, group, 0)
    hh = hh_ref[...]
    hl = hl_ref[...]

    many = together(sh.planes + 2)

    def pair(i, _):
        js = [i * many + k for k in range(many)]
        right = [right_transform(uh[j], ul[j], hh, hl) for j in js]
        parts = [split_bf16(x) for x in right]
        for j, (th, tl) in zip(js, parts):
            m[j] = left_transform(th, tl, hh, hl)
        return 0

    lax.fori_loop(0, (sh.planes + 2) // many, pair, 0)


def step_kernel(sh, stage, *refs):
    names = ["f", "carry", "rho", "scale", "hh", "hl", "gx", "gy", "gz", "r"]
    if stage > 0:
        names += ["coef", "z", "w"]
    if stage > 1:
        names += ["s", "q", "t"]
    last = stage == ITERS - 1
    if stage == 0:
        outs = ["z_new", "w_new"]
    elif last:
        outs = ["z_new"]
    else:
        outs = ["z_new", "w_new", "r_new", "s_new", "q_new", "t_new"]
        if stage == 1:
            outs.remove("s_new")
    outs += ["pay"] if last else ["f_new", "pay"]
    scratch = ["uh", "ul", "m"]
    if last:
        scratch += []
    k = dict(zip(names + outs + scratch, refs, strict=True))
    m = k["m"]
    emit_inverse(sh, k["f"], k["carry"], k["rho"], k["scale"], k["hh"], k["hl"], k["uh"], k["ul"], m)
    if stage > 0:
        alpha = k["coef"][1:2, :]
        beta = k["coef"][2:3, :]

    def plane(j, sums):
        here = m[j + 1]
        image = mass_rate * here + mean_conduct * stencil(
            sh, j, here, m[j], m[j + 2], k["gx"], k["gy"], k["gz"]
        )
        if stage == 0:
            z, w, r = here, image, k["r"][j]
        else:
            s, q, t = k["w"][j], here, image
            if stage > 1:
                s = s + beta * k["s"][j]
                q = q + beta * k["q"][j]
                t = t + beta * k["t"][j]
            r = k["r"][j] - alpha * s
            z = k["z"][j] - alpha * q
            w = k["w"][j] - alpha * t
            if not last:
                k["r_new"][j] = r
                k["q_new"][j] = q
                k["t_new"][j] = t
                if stage > 1:
                    k["s_new"][j] = s
        k["z_new"][j] = z
        if not last:
            k["w_new"][j] = w
        return (sums[0] + fold(sh, r * z), sums[1] + fold(sh, w * z))

    zero = jnp.zeros((SUB, sh.gz), jnp.float32)
    scal = scal_tile(sh, lax.fori_loop(0, sh.planes, plane, (zero, zero)))
    if last:
        pay = k["pay"]

        def spread(d, _):
            pay[d] = scal
            return 0

        lax.fori_loop(0, sh.devices, spread, 0)
    else:
        w_new = k["w_new"]
        emit_forward(sh, lambda j: w_new[j], k["rho"], k["hh"], k["hl"], k["f_new"], k["pay"], scal)


def finish_kernel(sh, *refs):
    coefs = refs[: ITERS - 1]
    recv = refs[ITERS - 1]
    u = refs[ITERS]
    fields = refs[ITERS + 1 : 2 * ITERS + 1]
    out = refs[-1]
    rows = [c[...] for c in coefs]
    rows.append(next_coefficients(sum_rows(sh.devices, recv, 0), rows[-1], sh.gz))
    weight = rows[-1][1:2]
    weights = [weight]
    for i in reversed(range(ITERS - 1)):
        weight = rows[i][1:2] + rows[i + 1][2:3] * weight
        weights.insert(0, weight)

    def plane(j, _):
        total = u[j]
        for weight, field in zip(weights, fields):
            total = total + weight * field[j]
        out[j] = total
        return 0

    lax.fori_loop(0, sh.planes, plane, 0)


def call(kernel, name, out_shapes, operands, scratch=(), aliases=None):
    whole = pl.BlockSpec(memory_space=VMEM)
    return pl.pallas_call(
        kernel,
        name=name,
        out_shape=[jax.ShapeDtypeStruct(s, jnp.float32) for s in out_shapes],
        in_specs=[whole] * len(operands),
        out_specs=[whole] * len(out_shapes),
        scratch_shapes=list(scratch),
        input_output_aliases=aliases or {},
        compiler_params=pltpu.CompilerParams(vmem_limit_bytes=12 * 1024 * 1024),
    )(*operands)


def exchange(x):
    return lax.all_to_all(x, AXES, split_axis=0, concat_axis=0, tiled=True)


def neighbours(first, final, axes):
    count = lax.axis_size(axes)
    return (
        lax.ppermute(final, axes, [(i, (i + 1) % count) for i in range(count)]),
        lax.ppermute(first, axes, [((i + 1) % count, i) for i in range(count)]),
    )


def local(potential, recovery, stimulus, conductivity):
    parts = lax.axis_size("py")
    devices = lax.axis_size("px") * parts
    planes, gy, gz = potential.shape
    sh = Shape(planes, gy, gz, devices)

    rho, scale, block, closure = mode_tables(sh.gx, gy, gz, planes)
    groups = gy // SUB

    def own_tiles(table):
        tiles = table.astype(np.float32).reshape(groups, SUB, sh.halves, LANE).transpose(0, 2, 1, 3)
        both = np.concatenate([tiles, tiles], axis=1).reshape(devices, sh.rows, LANE)
        return lax.dynamic_index_in_dim(jnp.asarray(both), lax.axis_index(AXES), 0, False)

    block = own_tiles(block)
    closure = own_tiles(closure)
    slot = lax.axis_index(AXES) * sh.slots + jnp.arange(sh.rows, dtype=jnp.int32)[:, None] // SUB
    onward = jnp.broadcast_to(
        (slot % sh.per_group < sh.halves).astype(jnp.float32), (sh.rows, LANE)
    )
    rho = jnp.asarray(rho.astype(np.float32))
    scale = jnp.asarray(scale.astype(np.float32))
    hh, hl = (jnp.asarray(x) for x in cas_parts(gy))

    coef = jnp.zeros((SUB, gz), jnp.float32)
    conductivity, block, closure, onward, coef = lax.optimization_barrier(
        (conductivity, block, closure, onward, coef)
    )
    wide = conductivity.shape[1]
    craw = lax.all_to_all(
        conductivity.reshape(parts, planes, wide, gz), "py", split_axis=0, concat_axis=0, tiled=True
    )
    drive = (
        excite_gain * potential * (potential - threshold) * (1.0 - potential) - potential * recovery
    )
    v_star = potential + time_step * (drive + stimulus)
    rate = base_rate + rate_slope * recovery / (potential + rate_shift)
    recovery_next = recovery + time_step * rate * (
        -recovery - excite_gain * potential * (potential - threshold - 1.0)
    )
    ulo, uhi = neighbours(v_star[:1], v_star[-1:], AXES)

    def edge(j):
        return craw[:, j].reshape(1, gy, gz)

    clo, chi = neighbours(edge(0), edge(planes - 1), AXES)

    slab = (planes, gy, gz)
    payload = (devices, sh.rows + SUB, LANE)
    carries = (devices, sh.rows, LANE)
    tables = [rho, hh, hl]
    gxf, gyf, gzf, r, f, pay = call(
        functools.partial(start_kernel, sh, parts),
        "start",
        [(planes + 1, gy, gz), slab, slab, slab, slab, payload],
        [v_star, ulo, uhi, craw, clo, chi] + tables,
        [pltpu.VMEM(slab, jnp.float32)],
    )
    spectral = [
        pltpu.VMEM((planes + 2, gy, gz), jnp.bfloat16),
        pltpu.VMEM((planes + 2, gy, gz), jnp.bfloat16),
        pltpu.VMEM((planes + 2, gy, gz), jnp.float32),
    ]
    coefs = []
    basis = []
    z = w = s = q = t = None
    for stage in range(ITERS):
        recv = exchange(pay)
        if stage == 0:
            (carry,) = call(
                functools.partial(scan_kernel, sh, True),
                "scan0",
                [carries],
                [recv, block, closure, onward],
            )
        else:
            carry, coef = call(
                functools.partial(scan_kernel, sh, False),
                f"scan{stage}",
                [carries, (SUB, gz)],
                [recv, block, closure, onward, coef],
            )
            coefs.append(coef)
        carry = exchange(carry)
        operands = [f, carry, rho, scale, hh, hl, gxf, gyf, gzf, r]
        if stage > 0:
            operands += [coef, z, w]
        if stage > 1:
            operands += [s, q, t]
        kernel = functools.partial(step_kernel, sh, stage)
        if stage == 0:
            z, w, f, pay = call(kernel, "step0", [slab, slab, slab, payload], operands, spectral)
        elif stage < ITERS - 1:
            shapes = [slab] * (5 if stage == 1 else 6) + [slab, payload]
            old_w = w
            results = call(kernel, f"step{stage}", shapes, operands, spectral)
            if stage == 1:
                z, w, r, q, t, f, pay = results
                s = old_w
            else:
                z, w, r, s, q, t, f, pay = results
        else:
            z, pay = call(kernel, f"step{stage}", [slab, (devices, SUB, LANE)], operands, spectral)
        basis.append(z)
    recv = exchange(pay)
    (potential_next,) = call(
        functools.partial(finish_kernel, sh), "finish", [slab], coefs + [recv, v_star] + basis
    )
    return potential_next, recovery_next


def solution(mesh):
    in_specs = (
        P(AXES, None, None),
        P(AXES, None, None),
        P(AXES, None, None),
        P("px", "py", None),
    )
    out_specs = (P(AXES, None, None), P(AXES, None, None))
    return jax.shard_map(local, mesh=mesh, in_specs=in_specs, out_specs=out_specs, check_vma=False)
```

```python
import functools
import math

import jax
import jax.numpy as jnp
import numpy as np
from jax import lax
from jax.experimental import pallas as pl
from jax.experimental.pallas import tpu as pltpu
from jax.sharding import PartitionSpec as P

ITERS = 4
mass_rate = 0.01
mean_conduct = 1.0
excite_gain = 8.0
threshold = 0.15
base_rate = 0.002
rate_slope = 0.2
rate_shift = 0.3
time_step = 0.1
alpha_low = 0.199
alpha_high = 5.03

AXES = ("px", "py")
SUB = 8
LANE = 128
VMEM = pltpu.MemorySpace.VMEM


def cas_parts(length):
    steps = np.arange(length)
    angle = 2.0 * np.pi / length * (steps[:, None] * steps[None, :] % length)
    table = np.cos(angle) + np.sin(angle)
    high = table.astype(jnp.bfloat16)
    low = (table - high.astype(np.float64)).astype(jnp.bfloat16)
    return high, low


def wave_term(length):
    return 2.0 - 2.0 * np.cos(2.0 * np.pi / length * np.arange(length))


def mode_tables(gx, gy, gz, planes):
    sigma = mass_rate / mean_conduct + wave_term(gy)[:, None] + wave_term(gz)[None, :]
    rho = 1.0 / (1.0 + 0.5 * sigma + np.sqrt(sigma + 0.25 * sigma * sigma))
    scale = rho / (1.0 - rho * rho) / (mean_conduct * gy * gz)
    block = rho**planes
    closure = 1.0 / (1.0 - rho**gx)
    return rho, scale, block, closure


def split_bf16(x):
    high = x.astype(jnp.bfloat16)
    low = (x - high.astype(jnp.float32)).astype(jnp.bfloat16)
    return high, low


def dot(a, b):
    return jnp.dot(a, b, preferred_element_type=jnp.float32)


def right_transform(xh, xl, hh, hl):
    return dot(xh, hh) + dot(xl, hh) + dot(xh, hl)


def left_transform(xh, xl, hh, hl):
    return dot(hh, xh) + dot(hh, xl) + dot(hl, xh)


def together(count):
    return max(k for k in range(1, 6) if count % k == 0)


class Shape:
    def __init__(self, planes, gy, gz, devices):
        self.planes, self.gy, self.gz, self.devices = planes, gy, gz, devices
        self.gx = planes * devices
        self.chips = devices // 2
        self.halves = gz // LANE
        self.per_group = 2 * self.halves
        self.groups = gy // SUB // 2
        self.tiles = self.groups * self.per_group
        self.slots = self.tiles // self.chips
        assert self.per_group % self.slots == 0
        self.rows = self.slots * SUB

    def tile(self, group, kind, half):
        return group * self.per_group + kind * self.halves + half

    def place(self, group, kind, half):
        q = kind * self.halves + half
        return group * (self.per_group // self.slots) + q // self.slots, q % self.slots * SUB


def emit_forward(sh, source, core, rho, hh_ref, hl_ref, f_ref, keep_ref, send_ref, scal):
    hh = hh_ref[...]
    hl = hl_ref[...]

    many = together(sh.planes)

    def pair(i, _):
        js = [i * many + k for k in range(many)]
        src = [split_bf16(source(j)) for j in js]
        right = [right_transform(xh, xl, hh, hl) for xh, xl in src]
        parts = [split_bf16(x) for x in right]
        for j, (th, tl) in zip(js, parts):
            f_ref[j] = left_transform(th, tl, hh, hl)
        return 0

    lax.fori_loop(0, sh.planes // many, pair, 0)

    for side, ref in ((core, keep_ref), (1 - core, send_ref)):

        def group(g, _, side=side, ref=ref):
            row = pl.multiple_of((side * sh.groups + g) * SUB, SUB)
            for half in range(sh.halves):
                lanes = slice(half * LANE, (half + 1) * LANE)
                decay = rho[pl.ds(row, SUB), lanes]
                f = [f_ref[j, pl.ds(row, SUB), lanes] for j in range(sh.planes)]
                p = f[0]
                e = f[-1]
                for j in range(1, sh.planes):
                    p = f[j] + decay * p
                    e = f[sh.planes - 1 - j] + decay * e
                ref[sh.tile(g, 0, half)] = p
                ref[sh.tile(g, 1, half)] = e
            return 0

        lax.fori_loop(0, sh.groups, group, 0, unroll=2)
        ref[sh.tiles] = scal


def join_kernel(sh, core_ref, keep, other, block, out):
    core = core_ref[0]
    early = core == 0
    scal = keep[sh.tiles] + other[sh.tiles]

    def group(g, _):
        row = pl.multiple_of((core * sh.groups + g) * SUB, SUB)
        for half in range(sh.halves):
            a = block[pl.ds(row, SUB), half * LANE : (half + 1) * LANE]
            for kind in range(2):
                at = sh.tile(g, kind, half)
                mine, its = keep[at], other[at]
                first = jnp.where(early, mine, its)
                second = jnp.where(early, its, mine)
                d, to = sh.place(g, kind, half)
                value = a * first + second if kind == 0 else first + a * second
                out[d, pl.ds(to, SUB), :] = value
        return 0

    lax.fori_loop(0, sh.groups, group, 0, unroll=4)

    def spread(d, _):
        out[d, pl.ds(sh.rows, SUB), :] = scal
        return 0

    lax.fori_loop(0, sh.chips, spread, 0, unroll=4)


def part_kernel(sh, core_ref, carry, keep, other, block, own, send):
    core = core_ref[0]
    early = core == 0

    def group(g, _):
        row = pl.multiple_of((core * sh.groups + g) * SUB, SUB)
        for half in range(sh.halves):
            a = block[pl.ds(row, SUB), half * LANE : (half + 1) * LANE]
            for kind in range(2):
                at = sh.tile(g, kind, half)
                mine, its = keep[at], other[at]
                d, to = sh.place(g, kind, half)
                outer = carry[d, pl.ds(to, SUB), :]
                if kind == 0:
                    inner = jnp.where(early, mine, its) + a * outer
                    own[at] = jnp.where(early, outer, inner)
                    send[at] = jnp.where(early, inner, outer)
                else:
                    inner = jnp.where(early, its, mine) + a * outer
                    own[at] = jnp.where(early, inner, outer)
                    send[at] = jnp.where(early, outer, inner)
        return 0

    lax.fori_loop(0, sh.groups, group, 0, unroll=4)


def stencil(sh, j, here, before, after, gx_ref, gy_ref, gz_ref):
    acc = gx_ref[j + 1] * (here - after) - gx_ref[j] * (before - here)
    flux = gy_ref[j] * (here - pltpu.roll(here, sh.gy - 1, 0))
    acc = acc + flux - pltpu.roll(flux, 1, 0)
    flux = gz_ref[j] * (here - pltpu.roll(here, sh.gz - 1, 1))
    return acc + flux - pltpu.roll(flux, 1, 1)


def fold(sh, x):
    return jnp.sum(x.reshape(sh.gy // SUB, SUB, sh.gz), axis=0)


def scal_tile(sh, parts):
    rows = []
    for part in parts:
        row = jnp.sum(part, axis=0, keepdims=True)
        total = row[:, :LANE]
        for half in range(1, sh.halves):
            total = total + row[:, half * LANE : (half + 1) * LANE]
        rows.append(total)
    rows.append(jnp.zeros((SUB - len(rows), LANE), jnp.float32))
    return jnp.concatenate(rows, axis=0)


def start_kernel(
    sh, parts, core_ref, u, ulo, uhi, craw, clo, chi, rho, hh, hl, gx, gy, gz, r, f, keep, send, c
):
    wide = sh.gy // parts
    for k in range(parts):
        c[:, k * wide : (k + 1) * wide, :] = 0.5 * craw[k]

    def faces(j, _):
        own = c[j]
        gy[j] = own + pltpu.roll(own, sh.gy - 1, 0)
        gz[j] = own + pltpu.roll(own, sh.gz - 1, 1)
        return 0

    lax.fori_loop(0, sh.planes, faces, 0)
    gx[0] = 0.5 * clo[0] + c[0]
    gx[sh.planes] = 0.5 * chi[0] + c[sh.planes - 1]

    def cross(j, _):
        gx[j] = c[j - 1] + c[j]
        return 0

    lax.fori_loop(1, sh.planes, cross, 0)

    last = sh.planes - 1
    r[0] = -stencil(sh, 0, u[0], ulo[0], u[1], gx, gy, gz)

    def inner(j, _):
        r[j] = -stencil(sh, j, u[j], u[j - 1], u[j + 1], gx, gy, gz)
        return 0

    lax.fori_loop(1, last, inner, 0)
    r[last] = -stencil(sh, last, u[last], u[last - 1], uhi[0], gx, gy, gz)
    scal = jnp.zeros((SUB, LANE), jnp.float32)
    emit_forward(sh, lambda j: r[j], core_ref[0], rho, hh, hl, f, keep, send, scal)


def scan_kernel(sh, first, *refs):
    recv, decay, closure, onward = refs[:4]
    if first:
        (out,) = refs[4:]
    else:
        coef, out, coef_out = refs[4:]
    count = sh.chips

    def run(rows, forward, store):
        a = decay[rows]
        order = (lambda i: i) if forward else (lambda i: count - 1 - i)

        def total(i, s):
            return recv[order(i), rows, :] + a * s

        zero = jnp.zeros(a.shape, jnp.float32)
        carry = lax.fori_loop(0, count, total, zero, unroll=8) * closure[rows]

        def step(i, carry):
            store(order(i), carry)
            return recv[order(i), rows, :] + a * carry

        lax.fori_loop(0, count, step, carry, unroll=8)

    if sh.slots == sh.per_group:
        half = sh.rows // 2
        for rows, forward in ((slice(0, half), True), (slice(half, sh.rows), False)):

            def store(d, x, rows=rows):
                out[d, rows, :] = x

            run(rows, forward, store)
    else:
        rows = slice(0, sh.rows)
        take = onward[...]

        def store_forward(d, x):
            out[d] = x

        def store_backward(d, x):
            out[d] = jnp.where(take > 0.5, out[d], x)

        run(rows, True, store_forward)
        run(rows, False, store_backward)

    if not first:
        sums = sum_rows(sh.chips, recv, sh.rows)
        coef_out[...] = next_coefficients(sums, coef[...], sh.gz)


def sum_rows(count, recv, at):
    def add(d, s):
        return s + recv[d, at : at + SUB, :]

    return lax.fori_loop(1, count, add, recv[0, at : at + SUB, :], unroll=4)


def next_coefficients(sums, previous, width):
    product = jnp.maximum(jnp.sum(sums[0:1], axis=1, keepdims=True), 0.0)
    curve = jnp.sum(sums[1:2], axis=1, keepdims=True)
    product = jnp.broadcast_to(product, (1, width))
    curve = jnp.broadcast_to(curve, (1, width))
    old_product = previous[0:1]
    old_alpha = previous[1:2]
    started = old_product > 0.0
    beta = jnp.where(started, product / jnp.where(started, old_product, 1.0), 0.0)
    curve = curve - beta * product / jnp.where(old_alpha > 0.0, old_alpha, 1.0)
    usable = curve > 0.0
    alpha = jnp.where(usable, product / jnp.where(usable, curve, 1.0), alpha_low)
    alpha = jnp.clip(alpha, alpha_low, alpha_high)
    return jnp.concatenate(
        [product, alpha, beta, jnp.zeros((SUB - 3, width), jnp.float32)], axis=0
    )


def emit_inverse(sh, core, f, own, other, rho, scale, hh_ref, hl_ref, uh, ul, m):
    tall = 2 * SUB
    for side, carry in ((core, own), (1 - core, other)):

        def group(i, _, side=side, carry=carry):
            row = pl.multiple_of(side * (sh.groups * SUB) + i * tall, tall)
            for half in range(sh.halves):
                lanes = slice(half * LANE, (half + 1) * LANE)
                decay = rho[pl.ds(row, tall), lanes]
                gain = scale[pl.ds(row, tall), lanes]
                first, final = (
                    jnp.concatenate(
                        [carry[sh.tile(g, kind, half)] for g in (2 * i, 2 * i + 1)], axis=0
                    )
                    for kind in range(2)
                )

                def put(j, value):
                    high, low = split_bf16(gain * value)
                    uh[j, pl.ds(row, tall), lanes] = high
                    ul[j, pl.ds(row, tall), lanes] = low

                fields = [f[j, pl.ds(row, tall), lanes] for j in range(sh.planes)]
                back = [None] * sh.planes
                e = final
                for j in reversed(range(sh.planes)):
                    back[j] = decay * e
                    e = fields[j] + back[j]
                put(0, first + decay * e)
                p = first
                for j in range(sh.planes):
                    p = fields[j] + decay * p
                    put(j + 1, p + back[j])
                put(sh.planes + 1, decay * p + final)
            return 0

        lax.fori_loop(0, sh.groups // 2, group, 0)
    hh = hh_ref[...]
    hl = hl_ref[...]

    many = together(sh.planes + 2)

    def pair(i, _):
        js = [i * many + k for k in range(many)]
        right = [right_transform(uh[j], ul[j], hh, hl) for j in js]
        parts = [split_bf16(x) for x in right]
        for j, (th, tl) in zip(js, parts):
            m[j] = left_transform(th, tl, hh, hl)
        return 0

    lax.fori_loop(0, (sh.planes + 2) // many, pair, 0)


def step_kernel(sh, stage, *refs):
    names = ["core", "f", "own", "other", "rho", "scale", "hh", "hl", "gx", "gy", "gz", "r"]
    if stage > 0:
        names += ["coef", "z", "w"]
    if stage > 1:
        names += ["s", "q", "t"]
    last = stage == ITERS - 1
    if stage == 0:
        outs = ["z_new", "w_new"]
    elif last:
        outs = ["z_new"]
    else:
        outs = ["z_new", "w_new", "r_new", "s_new", "q_new", "t_new"]
        if stage == 1:
            outs.remove("s_new")
    outs += ["pay"] if last else ["f_new", "keep", "send"]
    scratch = ["uh", "ul", "m"]
    k = dict(zip(names + outs + scratch, refs, strict=True))
    m = k["m"]
    core = k["core"][0]
    tables = (k["rho"], k["scale"], k["hh"], k["hl"])
    emit_inverse(sh, core, k["f"], k["own"], k["other"], *tables, k["uh"], k["ul"], m)
    if stage > 0:
        alpha = k["coef"][1:2, :]
        beta = k["coef"][2:3, :]

    def plane(j, sums):
        here = m[j + 1]
        image = mass_rate * here + mean_conduct * stencil(
            sh, j, here, m[j], m[j + 2], k["gx"], k["gy"], k["gz"]
        )
        if stage == 0:
            z, w, r = here, image, k["r"][j]
        else:
            s, q, t = k["w"][j], here, image
            if stage > 1:
                s = s + beta * k["s"][j]
                q = q + beta * k["q"][j]
                t = t + beta * k["t"][j]
            r = k["r"][j] - alpha * s
            z = k["z"][j] - alpha * q
            w = k["w"][j] - alpha * t
            if not last:
                k["r_new"][j] = r
                k["q_new"][j] = q
                k["t_new"][j] = t
                if stage > 1:
                    k["s_new"][j] = s
        k["z_new"][j] = z
        if not last:
            k["w_new"][j] = w
        return (sums[0] + fold(sh, r * z), sums[1] + fold(sh, w * z))

    zero = jnp.zeros((SUB, sh.gz), jnp.float32)
    scal = scal_tile(sh, lax.fori_loop(0, sh.planes, plane, (zero, zero)))
    if last:
        pay = k["pay"]

        def spread(d, _):
            pay[d] = scal
            return 0

        lax.fori_loop(0, sh.devices, spread, 0)
    else:
        w_new = k["w_new"]
        into = (k["f_new"], k["keep"], k["send"])
        emit_forward(sh, lambda j: w_new[j], core, k["rho"], k["hh"], k["hl"], *into, scal)


def finish_kernel(sh, *refs):
    coefs = refs[: ITERS - 1]
    recv = refs[ITERS - 1]
    u = refs[ITERS]
    fields = refs[ITERS + 1 : 2 * ITERS + 1]
    out = refs[-1]
    rows = [c[...] for c in coefs]
    rows.append(next_coefficients(sum_rows(sh.devices, recv, 0), rows[-1], sh.gz))
    weight = rows[-1][1:2]
    weights = [weight]
    for i in reversed(range(ITERS - 1)):
        weight = rows[i][1:2] + rows[i + 1][2:3] * weight
        weights.insert(0, weight)

    def plane(j, _):
        total = u[j]
        for weight, field in zip(weights, fields):
            total = total + weight * field[j]
        out[j] = total
        return 0

    lax.fori_loop(0, sh.planes, plane, 0)


def call(kernel, name, out_shapes, operands, scratch=(), aliases=None):
    whole = pl.BlockSpec(memory_space=VMEM)
    return pl.pallas_call(
        kernel,
        name=name,
        out_shape=[jax.ShapeDtypeStruct(s, jnp.float32) for s in out_shapes],
        in_specs=[
            pl.BlockSpec(memory_space=pltpu.MemorySpace.SMEM) if x.dtype == jnp.int32 else whole
            for x in operands
        ],
        out_specs=[whole] * len(out_shapes),
        scratch_shapes=list(scratch),
        input_output_aliases=aliases or {},
        compiler_params=pltpu.CompilerParams(vmem_limit_bytes=12 * 1024 * 1024),
    )(*operands)


def exchange(x, groups=None):
    return lax.all_to_all(
        x, AXES, split_axis=0, concat_axis=0, tiled=True, axis_index_groups=groups
    )


def neighbours(first, final, axes):
    count = lax.axis_size(axes)
    return (
        lax.ppermute(final, axes, [(i, (i + 1) % count) for i in range(count)]),
        lax.ppermute(first, axes, [((i + 1) % count, i) for i in range(count)]),
    )


def local(potential, recovery, stimulus, conductivity):
    parts = lax.axis_size("py")
    devices = lax.axis_size("px") * parts
    planes, gy, gz = potential.shape
    sh = Shape(planes, gy, gz, devices)

    rho, scale, block, closure = mode_tables(sh.gx, gy, gz, planes)
    groups = gy // SUB

    def own_tiles(table):
        tiles = table.astype(np.float32).reshape(groups, SUB, sh.halves, LANE).transpose(0, 2, 1, 3)
        both = np.concatenate([tiles, tiles], axis=1).reshape(2, sh.chips, sh.rows, LANE)
        both = both.transpose(1, 0, 2, 3).reshape(devices, sh.rows, LANE)
        return lax.dynamic_index_in_dim(jnp.asarray(both), lax.axis_index(AXES), 0, False)

    across = jnp.asarray(block.astype(np.float32))
    block = own_tiles(block * block)
    closure = own_tiles(closure)
    core = jnp.reshape(lax.axis_index(AXES) % 2, (1,))
    slot = lax.axis_index(AXES) // 2 * sh.slots + jnp.arange(sh.rows, dtype=jnp.int32)[:, None] // SUB
    onward = jnp.broadcast_to(
        (slot % sh.per_group < sh.halves).astype(jnp.float32), (sh.rows, LANE)
    )
    rho = jnp.asarray(rho.astype(np.float32))
    scale = jnp.asarray(scale.astype(np.float32))
    hh, hl = (jnp.asarray(x) for x in cas_parts(gy))

    coef = jnp.zeros((SUB, gz), jnp.float32)
    conductivity, block, closure, onward, coef, core = lax.optimization_barrier(
        (conductivity, block, closure, onward, coef, core)
    )
    wide = conductivity.shape[1]
    craw = lax.all_to_all(
        conductivity.reshape(parts, planes, wide, gz), "py", split_axis=0, concat_axis=0, tiled=True
    )
    drive = (
        excite_gain * potential * (potential - threshold) * (1.0 - potential) - potential * recovery
    )
    v_star = potential + time_step * (drive + stimulus)
    rate = base_rate + rate_slope * recovery / (potential + rate_shift)
    recovery_next = recovery + time_step * rate * (
        -recovery - excite_gain * potential * (potential - threshold - 1.0)
    )
    ulo, uhi = neighbours(v_star[:1], v_star[-1:], AXES)

    def edge(j):
        return craw[:, j].reshape(1, gy, gz)

    clo, chi = neighbours(edge(0), edge(planes - 1), AXES)

    slab = (planes, gy, gz)
    payload = (sh.chips, sh.rows + SUB, LANE)
    carries = (sh.chips, sh.rows, LANE)
    sums = (sh.tiles + 1, SUB, LANE)
    parted = (sh.tiles, SUB, LANE)
    swap = [(i, i ^ 1) for i in range(devices)]
    same_core = [[2 * chip + side for chip in range(sh.chips)] for side in range(2)]
    tables = [rho, hh, hl]
    gxf, gyf, gzf, r, f, keep, send = call(
        functools.partial(start_kernel, sh, parts),
        "start",
        [(planes + 1, gy, gz), slab, slab, slab, slab, sums, sums],
        [core, v_star, ulo, uhi, craw, clo, chi] + tables,
        [pltpu.VMEM(slab, jnp.float32)],
    )
    spectral = [
        pltpu.VMEM((planes + 2, gy, gz), jnp.bfloat16),
        pltpu.VMEM((planes + 2, gy, gz), jnp.bfloat16),
        pltpu.VMEM((planes + 2, gy, gz), jnp.float32),
    ]
    coefs = []
    basis = []
    z = w = s = q = t = None
    for stage in range(ITERS):
        other = lax.ppermute(send, AXES, swap)
        (pay,) = call(
            functools.partial(join_kernel, sh), f"join{stage}", [payload], [core, keep, other, across]
        )
        recv = exchange(pay, same_core)
        if stage == 0:
            (carry,) = call(
                functools.partial(scan_kernel, sh, True),
                "scan0",
                [carries],
                [recv, block, closure, onward],
            )
        else:
            carry, coef = call(
                functools.partial(scan_kernel, sh, False),
                f"scan{stage}",
                [carries, (SUB, gz)],
                [recv, block, closure, onward, coef],
            )
            coefs.append(coef)
        carry = exchange(carry, same_core)
        own, send = call(
            functools.partial(part_kernel, sh),
            f"part{stage}",
            [parted, parted],
            [core, carry, keep, other, across],
        )
        other = lax.ppermute(send, AXES, swap)
        operands = [core, f, own, other, rho, scale, hh, hl, gxf, gyf, gzf, r]
        if stage > 0:
            operands += [coef, z, w]
        if stage > 1:
            operands += [s, q, t]
        kernel = functools.partial(step_kernel, sh, stage)
        if stage == 0:
            shapes = [slab, slab, slab, sums, sums]
            z, w, f, keep, send = call(kernel, "step0", shapes, operands, spectral)
        elif stage < ITERS - 1:
            shapes = [slab] * (5 if stage == 1 else 6) + [slab, sums, sums]
            old_w = w
            results = call(kernel, f"step{stage}", shapes, operands, spectral)
            if stage == 1:
                z, w, r, q, t, f, keep, send = results
                s = old_w
            else:
                z, w, r, s, q, t, f, keep, send = results
        else:
            z, pay = call(kernel, f"step{stage}", [slab, (devices, SUB, LANE)], operands, spectral)
        basis.append(z)
    recv = exchange(pay)
    (potential_next,) = call(
        functools.partial(finish_kernel, sh), "finish", [slab], coefs + [recv, v_star] + basis
    )
    return potential_next, recovery_next


def solution(mesh):
    in_specs = (
        P(AXES, None, None),
        P(AXES, None, None),
        P(AXES, None, None),
        P("px", "py", None),
    )
    out_specs = (P(AXES, None, None), P(AXES, None, None))
    return jax.shard_map(local, mesh=mesh, in_specs=in_specs, out_specs=out_specs, check_vma=False)
```

```python
import functools
import math

import jax
import jax.numpy as jnp
import numpy as np
from jax import lax
from jax.experimental import pallas as pl
from jax.experimental.pallas import tpu as pltpu
from jax.sharding import PartitionSpec as P

ITERS = 4
mass_rate = 0.01
mean_conduct = 1.0
excite_gain = 8.0
threshold = 0.15
base_rate = 0.002
rate_slope = 0.2
rate_shift = 0.3
time_step = 0.1
alpha_low = 0.199
alpha_high = 5.03

AXES = ("px", "py")
SUB = 8
LANE = 128
VMEM = pltpu.MemorySpace.VMEM


def cas_parts(length):
    steps = np.arange(length)
    angle = 2.0 * np.pi / length * (steps[:, None] * steps[None, :] % length)
    table = np.cos(angle) + np.sin(angle)
    high = table.astype(jnp.bfloat16)
    low = (table - high.astype(np.float64)).astype(jnp.bfloat16)
    return high, low


def wave_term(length):
    return 2.0 - 2.0 * np.cos(2.0 * np.pi / length * np.arange(length))


def mode_tables(gx, gy, gz, planes):
    sigma = mass_rate / mean_conduct + wave_term(gy)[:, None] + wave_term(gz)[None, :]
    rho = 1.0 / (1.0 + 0.5 * sigma + np.sqrt(sigma + 0.25 * sigma * sigma))
    scale = rho / (1.0 - rho * rho) / (mean_conduct * gy * gz)
    block = rho**planes
    closure = 1.0 / (1.0 - rho**gx)
    return rho, scale, block, closure


def split_bf16(x):
    high = x.astype(jnp.bfloat16)
    low = (x - high.astype(jnp.float32)).astype(jnp.bfloat16)
    return high, low


def dot(a, b):
    return jnp.dot(a, b, preferred_element_type=jnp.float32)


def right_transform(xh, xl, hh, hl):
    return dot(xh, hh) + dot(xl, hh) + dot(xh, hl)


def left_transform(xh, xl, hh, hl):
    return dot(hh, xh) + dot(hh, xl) + dot(hl, xh)


def together(count):
    return max(k for k in range(1, 6) if count % k == 0)


class Shape:
    def __init__(self, planes, gy, gz, devices):
        self.planes, self.gy, self.gz, self.devices = planes, gy, gz, devices
        self.gx = planes * devices
        self.chips = devices // 2
        self.halves = gz // LANE
        self.per_group = 2 * self.halves
        self.groups = gy // SUB // 2
        self.tiles = self.groups * self.per_group
        self.slots = self.tiles // self.chips
        assert self.per_group % self.slots == 0
        self.rows = self.slots * SUB

    def tile(self, group, kind, half):
        return group * self.per_group + kind * self.halves + half

    def place(self, group, kind, half):
        q = kind * self.halves + half
        return group * (self.per_group // self.slots) + q // self.slots, q % self.slots * SUB


def emit_forward(sh, source, core, rho, hh_ref, hl_ref, f_ref, keep_ref, send_ref, scal):
    hh = hh_ref[...]
    hl = hl_ref[...]

    many = together(sh.planes)

    def pair(i, _):
        js = [i * many + k for k in range(many)]
        src = [split_bf16(source(j)) for j in js]
        right = [right_transform(xh, xl, hh, hl) for xh, xl in src]
        parts = [split_bf16(x) for x in right]
        for j, (th, tl) in zip(js, parts):
            f_ref[j] = left_transform(th, tl, hh, hl)
        return 0

    lax.fori_loop(0, sh.planes // many, pair, 0)

    for side, ref in ((core, keep_ref), (1 - core, send_ref)):

        def group(g, _, side=side, ref=ref):
            row = pl.multiple_of((side * sh.groups + g) * SUB, SUB)
            for half in range(sh.halves):
                lanes = slice(half * LANE, (half + 1) * LANE)
                decay = rho[pl.ds(row, SUB), lanes]
                f = [f_ref[j, pl.ds(row, SUB), lanes] for j in range(sh.planes)]
                p = f[0]
                e = f[-1]
                for j in range(1, sh.planes):
                    p = f[j] + decay * p
                    e = f[sh.planes - 1 - j] + decay * e
                ref[sh.tile(g, 0, half)] = p
                ref[sh.tile(g, 1, half)] = e
            return 0

        lax.fori_loop(0, sh.groups, group, 0, unroll=2)
        ref[sh.tiles] = scal


def join_kernel(sh, sums, core_ref, keep, other, block, out):
    core = core_ref[0]
    early = core == 0
    def group(g, _):
        row = pl.multiple_of((core * sh.groups + g) * SUB, SUB)
        for half in range(sh.halves):
            a = block[pl.ds(row, SUB), half * LANE : (half + 1) * LANE]
            for kind in range(2):
                at = sh.tile(g, kind, half)
                mine, its = keep[at], other[at]
                first = jnp.where(early, mine, its)
                second = jnp.where(early, its, mine)
                d, to = sh.place(g, kind, half)
                value = a * first + second if kind == 0 else first + a * second
                out[d, pl.ds(to, SUB), :] = value
        return 0

    lax.fori_loop(0, sh.groups, group, 0, unroll=4)

    if sums:
        scal = keep[sh.tiles] + other[sh.tiles]

        def spread(d, _):
            out[d, pl.ds(sh.rows, SUB), :] = scal
            return 0

        lax.fori_loop(0, sh.chips, spread, 0, unroll=4)


def part_kernel(sh, core_ref, carry, keep, other, block, own, send):
    core = core_ref[0]
    early = core == 0

    def group(g, _):
        row = pl.multiple_of((core * sh.groups + g) * SUB, SUB)
        for half in range(sh.halves):
            a = block[pl.ds(row, SUB), half * LANE : (half + 1) * LANE]
            for kind in range(2):
                at = sh.tile(g, kind, half)
                mine, its = keep[at], other[at]
                d, to = sh.place(g, kind, half)
                outer = carry[d, pl.ds(to, SUB), :]
                if kind == 0:
                    inner = jnp.where(early, mine, its) + a * outer
                    own[at] = jnp.where(early, outer, inner)
                    send[at] = jnp.where(early, inner, outer)
                else:
                    inner = jnp.where(early, its, mine) + a * outer
                    own[at] = jnp.where(early, inner, outer)
                    send[at] = jnp.where(early, outer, inner)
        return 0

    lax.fori_loop(0, sh.groups, group, 0, unroll=4)


def stencil(sh, j, here, before, after, gx_ref, gy_ref, gz_ref):
    acc = gx_ref[j + 1] * (here - after) - gx_ref[j] * (before - here)
    flux = gy_ref[j] * (here - pltpu.roll(here, sh.gy - 1, 0))
    acc = acc + flux - pltpu.roll(flux, 1, 0)
    flux = gz_ref[j] * (here - pltpu.roll(here, sh.gz - 1, 1))
    return acc + flux - pltpu.roll(flux, 1, 1)


def fold(sh, x):
    return jnp.sum(x.reshape(sh.gy // SUB, SUB, sh.gz), axis=0)


def scal_tile(sh, parts):
    rows = []
    for part in parts:
        row = jnp.sum(part, axis=0, keepdims=True)
        total = row[:, :LANE]
        for half in range(1, sh.halves):
            total = total + row[:, half * LANE : (half + 1) * LANE]
        rows.append(total)
    rows.append(jnp.zeros((SUB - len(rows), LANE), jnp.float32))
    return jnp.concatenate(rows, axis=0)


def edge_kernel(sh, parts, place_ref, *refs):
    pieces, (first, last) = refs[:parts], refs[parts:]
    wide = sh.gy // parts
    for k in range(parts):
        at = pl.multiple_of((place_ref[0] ^ k) * wide, wide)
        first[0, pl.ds(at, wide), :] = pieces[k][0]
        last[0, pl.ds(at, wide), :] = pieces[k][1]


def start_kernel(sh, parts, core_ref, place_ref, u, ulo, uhi, clo, chi, first, last, *refs):
    pieces = refs[: parts if sh.planes > 2 else 0]
    rho, hh, hl, gx, gy, gz, r, f, keep, send, c = refs[len(pieces) :]
    wide = sh.gy // parts
    c[0] = 0.5 * first[0]
    c[sh.planes - 1] = 0.5 * last[0]
    for k, piece in enumerate(pieces):
        at = pl.multiple_of((place_ref[0] ^ k) * wide, wide)
        c[1 : sh.planes - 1, pl.ds(at, wide), :] = 0.5 * piece[...]

    def faces(j, _):
        own = c[j]
        gy[j] = own + pltpu.roll(own, sh.gy - 1, 0)
        gz[j] = own + pltpu.roll(own, sh.gz - 1, 1)
        return 0

    lax.fori_loop(0, sh.planes, faces, 0)
    gx[0] = 0.5 * clo[0] + c[0]
    gx[sh.planes] = 0.5 * chi[0] + c[sh.planes - 1]

    def cross(j, _):
        gx[j] = c[j - 1] + c[j]
        return 0

    lax.fori_loop(1, sh.planes, cross, 0)

    end = sh.planes - 1
    r[0] = -stencil(sh, 0, u[0], ulo[0], u[1], gx, gy, gz)

    def inner(j, _):
        r[j] = -stencil(sh, j, u[j], u[j - 1], u[j + 1], gx, gy, gz)
        return 0

    lax.fori_loop(1, end, inner, 0)
    r[end] = -stencil(sh, end, u[end], u[end - 1], uhi[0], gx, gy, gz)
    scal = jnp.zeros((SUB, LANE), jnp.float32)
    emit_forward(sh, lambda j: r[j], core_ref[0], rho, hh, hl, f, keep, send, scal)


def scan_kernel(sh, first, *refs):
    recv, decay, closure, onward = refs[:4]
    if first:
        (out,) = refs[4:]
    else:
        coef, out, coef_out = refs[4:]
    count = sh.chips

    def run(rows, forward, store):
        a = decay[rows]
        order = (lambda i: i) if forward else (lambda i: count - 1 - i)

        def total(i, s):
            return recv[order(i), rows, :] + a * s

        zero = jnp.zeros(a.shape, jnp.float32)
        carry = lax.fori_loop(0, count, total, zero, unroll=8) * closure[rows]

        def step(i, carry):
            store(order(i), carry)
            return recv[order(i), rows, :] + a * carry

        lax.fori_loop(0, count, step, carry, unroll=8)

    if sh.slots == sh.per_group:
        half = sh.rows // 2
        for rows, forward in ((slice(0, half), True), (slice(half, sh.rows), False)):

            def store(d, x, rows=rows):
                out[d, rows, :] = x

            run(rows, forward, store)
    else:
        rows = slice(0, sh.rows)
        take = onward[...]

        def store_forward(d, x):
            out[d] = x

        def store_backward(d, x):
            out[d] = jnp.where(take > 0.5, out[d], x)

        run(rows, True, store_forward)
        run(rows, False, store_backward)

    if not first:
        sums = sum_rows(sh.chips, recv, sh.rows)
        coef_out[...] = next_coefficients(sums, coef[...], sh.gz)


def sum_rows(count, recv, at):
    def add(d, s):
        return s + recv[d, at : at + SUB, :]

    return lax.fori_loop(1, count, add, recv[0, at : at + SUB, :], unroll=4)


def next_coefficients(sums, previous, width):
    product = jnp.maximum(jnp.sum(sums[0:1], axis=1, keepdims=True), 0.0)
    curve = jnp.sum(sums[1:2], axis=1, keepdims=True)
    product = jnp.broadcast_to(product, (1, width))
    curve = jnp.broadcast_to(curve, (1, width))
    old_product = previous[0:1]
    old_alpha = previous[1:2]
    started = old_product > 0.0
    beta = jnp.where(started, product / jnp.where(started, old_product, 1.0), 0.0)
    curve = curve - beta * product / jnp.where(old_alpha > 0.0, old_alpha, 1.0)
    usable = curve > 0.0
    alpha = jnp.where(usable, product / jnp.where(usable, curve, 1.0), alpha_low)
    alpha = jnp.clip(alpha, alpha_low, alpha_high)
    return jnp.concatenate(
        [product, alpha, beta, jnp.zeros((SUB - 3, width), jnp.float32)], axis=0
    )


def emit_inverse(sh, core, f, own, other, rho, scale, hh_ref, hl_ref, uh, ul, m):
    tall = 2 * SUB
    for side, carry in ((core, own), (1 - core, other)):

        def group(i, _, side=side, carry=carry):
            row = pl.multiple_of(side * (sh.groups * SUB) + i * tall, tall)
            for half in range(sh.halves):
                lanes = slice(half * LANE, (half + 1) * LANE)
                decay = rho[pl.ds(row, tall), lanes]
                gain = scale[pl.ds(row, tall), lanes]
                first, final = (
                    jnp.concatenate(
                        [carry[sh.tile(g, kind, half)] for g in (2 * i, 2 * i + 1)], axis=0
                    )
                    for kind in range(2)
                )

                def put(j, value):
                    high, low = split_bf16(gain * value)
                    uh[j, pl.ds(row, tall), lanes] = high
                    ul[j, pl.ds(row, tall), lanes] = low

                fields = [f[j, pl.ds(row, tall), lanes] for j in range(sh.planes)]
                back = [None] * sh.planes
                e = final
                for j in reversed(range(sh.planes)):
                    back[j] = decay * e
                    e = fields[j] + back[j]
                put(0, first + decay * e)
                p = first
                for j in range(sh.planes):
                    p = fields[j] + decay * p
                    put(j + 1, p + back[j])
                put(sh.planes + 1, decay * p + final)
            return 0

        lax.fori_loop(0, sh.groups // 2, group, 0)
    hh = hh_ref[...]
    hl = hl_ref[...]

    many = together(sh.planes + 2)

    def pair(i, _):
        js = [i * many + k for k in range(many)]
        right = [right_transform(uh[j], ul[j], hh, hl) for j in js]
        parts = [split_bf16(x) for x in right]
        for j, (th, tl) in zip(js, parts):
            m[j] = left_transform(th, tl, hh, hl)
        return 0

    lax.fori_loop(0, (sh.planes + 2) // many, pair, 0)


def step_kernel(sh, stage, *refs):
    names = ["core", "f", "own", "other", "rho", "scale", "hh", "hl", "gx", "gy", "gz", "r"]
    if stage > 0:
        names += ["coef", "z", "w"]
    if stage > 1:
        names += ["s", "q", "t"]
    last = stage == ITERS - 1
    if stage == 0:
        outs = ["z_new", "w_new"]
    elif last:
        outs = ["z_new"]
    else:
        outs = ["z_new", "w_new", "r_new", "s_new", "q_new", "t_new"]
        if stage == 1:
            outs.remove("s_new")
    outs += ["pay"] if last else ["f_new", "keep", "send"]
    scratch = ["uh", "ul", "m"]
    k = dict(zip(names + outs + scratch, refs, strict=True))
    m = k["m"]
    core = k["core"][0]
    tables = (k["rho"], k["scale"], k["hh"], k["hl"])
    emit_inverse(sh, core, k["f"], k["own"], k["other"], *tables, k["uh"], k["ul"], m)
    if stage > 0:
        alpha = k["coef"][1:2, :]
        beta = k["coef"][2:3, :]

    def plane(j, sums):
        here = m[j + 1]
        image = mass_rate * here + mean_conduct * stencil(
            sh, j, here, m[j], m[j + 2], k["gx"], k["gy"], k["gz"]
        )
        if stage == 0:
            z, w, r = here, image, k["r"][j]
        else:
            s, q, t = k["w"][j], here, image
            if stage > 1:
                s = s + beta * k["s"][j]
                q = q + beta * k["q"][j]
                t = t + beta * k["t"][j]
            r = k["r"][j] - alpha * s
            z = k["z"][j] - alpha * q
            w = k["w"][j] - alpha * t
            if not last:
                k["r_new"][j] = r
                k["q_new"][j] = q
                k["t_new"][j] = t
                if stage > 1:
                    k["s_new"][j] = s
        k["z_new"][j] = z
        if not last:
            k["w_new"][j] = w
        return (sums[0] + fold(sh, r * z), sums[1] + fold(sh, w * z))

    zero = jnp.zeros((SUB, sh.gz), jnp.float32)
    scal = scal_tile(sh, lax.fori_loop(0, sh.planes, plane, (zero, zero)))
    if last:
        pay = k["pay"]

        def spread(d, _):
            pay[d] = scal
            return 0

        lax.fori_loop(0, sh.devices, spread, 0)
    else:
        w_new = k["w_new"]
        into = (k["f_new"], k["keep"], k["send"])
        emit_forward(sh, lambda j: w_new[j], core, k["rho"], k["hh"], k["hl"], *into, scal)


def finish_kernel(sh, *refs):
    coefs = refs[: ITERS - 1]
    recv = refs[ITERS - 1]
    u = refs[ITERS]
    fields = refs[ITERS + 1 : 2 * ITERS + 1]
    out = refs[-1]
    rows = [c[...] for c in coefs]
    rows.append(next_coefficients(sum_rows(sh.devices, recv, 0), rows[-1], sh.gz))
    weight = rows[-1][1:2]
    weights = [weight]
    for i in reversed(range(ITERS - 1)):
        weight = rows[i][1:2] + rows[i + 1][2:3] * weight
        weights.insert(0, weight)

    def plane(j, _):
        total = u[j]
        for weight, field in zip(weights, fields):
            total = total + weight * field[j]
        out[j] = total
        return 0

    lax.fori_loop(0, sh.planes, plane, 0)


def call(kernel, name, out_shapes, operands, scratch=(), aliases=None):
    whole = pl.BlockSpec(memory_space=VMEM)
    return pl.pallas_call(
        kernel,
        name=name,
        out_shape=[jax.ShapeDtypeStruct(s, jnp.float32) for s in out_shapes],
        in_specs=[
            pl.BlockSpec(memory_space=pltpu.MemorySpace.SMEM) if x.dtype == jnp.int32 else whole
            for x in operands
        ],
        out_specs=[whole] * len(out_shapes),
        scratch_shapes=list(scratch),
        input_output_aliases=aliases or {},
        compiler_params=pltpu.CompilerParams(vmem_limit_bytes=12 * 1024 * 1024),
    )(*operands)


def exchange(x, groups=None):
    return lax.all_to_all(
        x, AXES, split_axis=0, concat_axis=0, tiled=True, axis_index_groups=groups
    )


def neighbours(first, final, axes):
    count = lax.axis_size(axes)
    return (
        lax.ppermute(final, axes, [(i, (i + 1) % count) for i in range(count)]),
        lax.ppermute(first, axes, [((i + 1) % count, i) for i in range(count)]),
    )


def local(potential, recovery, stimulus, conductivity):
    parts = lax.axis_size("py")
    devices = lax.axis_size("px") * parts
    planes, gy, gz = potential.shape
    sh = Shape(planes, gy, gz, devices)

    rho, scale, block, closure = mode_tables(sh.gx, gy, gz, planes)
    groups = gy // SUB

    def own_tiles(table):
        tiles = table.astype(np.float32).reshape(groups, SUB, sh.halves, LANE).transpose(0, 2, 1, 3)
        both = np.concatenate([tiles, tiles], axis=1).reshape(2, sh.chips, sh.rows, LANE)
        both = both.transpose(1, 0, 2, 3).reshape(devices, sh.rows, LANE)
        return lax.dynamic_index_in_dim(jnp.asarray(both), lax.axis_index(AXES), 0, False)

    across = jnp.asarray(block.astype(np.float32))
    block = own_tiles(block * block)
    closure = own_tiles(closure)
    core = jnp.reshape(lax.axis_index(AXES) % 2, (1,))
    place = jnp.reshape(lax.axis_index("py"), (1,))
    slot = lax.axis_index(AXES) // 2 * sh.slots + jnp.arange(sh.rows, dtype=jnp.int32)[:, None] // SUB
    onward = jnp.broadcast_to(
        (slot % sh.per_group < sh.halves).astype(jnp.float32), (sh.rows, LANE)
    )
    rho = jnp.asarray(rho.astype(np.float32))
    scale = jnp.asarray(scale.astype(np.float32))
    hh, hl = (jnp.asarray(x) for x in cas_parts(gy))

    coef = jnp.zeros((SUB, gz), jnp.float32)
    conductivity, block, closure, onward, coef, core = lax.optimization_barrier(
        (conductivity, block, closure, onward, coef, core)
    )
    wide = conductivity.shape[1]
    blocks = conductivity.reshape(parts, planes, wide, gz)
    mine = lax.axis_index("py")
    pieces = [lax.dynamic_index_in_dim(blocks, mine ^ k, 0, False) for k in range(parts)]
    edges = [jnp.stack([x[0], x[planes - 1]]) for x in pieces]
    inner = [x[1 : planes - 1] for x in pieces] if planes > 2 else []

    def across_y(items):
        return [
            lax.ppermute(x, "py", [(i, i ^ k) for i in range(parts)]) if k else x
            for k, x in enumerate(items)
        ]

    edges = across_y(edges)
    inner = across_y(inner)
    drive = (
        excite_gain * potential * (potential - threshold) * (1.0 - potential) - potential * recovery
    )
    v_star = potential + time_step * (drive + stimulus)
    rate = base_rate + rate_slope * recovery / (potential + rate_shift)
    recovery_next = recovery + time_step * rate * (
        -recovery - excite_gain * potential * (potential - threshold - 1.0)
    )
    ulo, uhi = neighbours(v_star[:1], v_star[-1:], AXES)

    slab = (planes, gy, gz)
    payload = (sh.chips, sh.rows + SUB, LANE)
    carries = (sh.chips, sh.rows, LANE)
    sums = (sh.tiles + 1, SUB, LANE)
    parted = (sh.tiles, SUB, LANE)
    swap = [(i, i ^ 1) for i in range(devices)]
    same_core = [[2 * chip + side for chip in range(sh.chips)] for side in range(2)]
    tables = [rho, hh, hl]
    plane = (1, gy, gz)
    first, last = call(
        functools.partial(edge_kernel, sh, parts), "edges", [plane, plane], [place] + edges
    )
    clo, chi = neighbours(first, last, AXES)
    gxf, gyf, gzf, r, f, keep, send = call(
        functools.partial(start_kernel, sh, parts),
        "start",
        [(planes + 1, gy, gz), slab, slab, slab, slab, sums, sums],
        [core, place, v_star, ulo, uhi, clo, chi, first, last] + inner + tables,
        [pltpu.VMEM(slab, jnp.float32)],
    )
    spectral = [
        pltpu.VMEM((planes + 2, gy, gz), jnp.bfloat16),
        pltpu.VMEM((planes + 2, gy, gz), jnp.bfloat16),
        pltpu.VMEM((planes + 2, gy, gz), jnp.float32),
    ]
    coefs = []
    basis = []
    z = w = s = q = t = None
    for stage in range(ITERS):
        other = lax.ppermute(send, AXES, swap)
        (pay,) = call(
            functools.partial(join_kernel, sh, stage > 0),
            f"join{stage}",
            [payload if stage > 0 else carries],
            [core, keep, other, across],
        )
        recv = exchange(pay, same_core)
        if stage == 0:
            (carry,) = call(
                functools.partial(scan_kernel, sh, True),
                "scan0",
                [carries],
                [recv, block, closure, onward],
            )
        else:
            carry, coef = call(
                functools.partial(scan_kernel, sh, False),
                f"scan{stage}",
                [carries, (SUB, gz)],
                [recv, block, closure, onward, coef],
            )
            coefs.append(coef)
        carry = exchange(carry, same_core)
        own, send = call(
            functools.partial(part_kernel, sh),
            f"part{stage}",
            [parted, parted],
            [core, carry, keep, other, across],
        )
        other = lax.ppermute(send, AXES, swap)
        operands = [core, f, own, other, rho, scale, hh, hl, gxf, gyf, gzf, r]
        if stage > 0:
            operands += [coef, z, w]
        if stage > 1:
            operands += [s, q, t]
        kernel = functools.partial(step_kernel, sh, stage)
        if stage == 0:
            shapes = [slab, slab, slab, sums, sums]
            z, w, f, keep, send = call(kernel, "step0", shapes, operands, spectral)
        elif stage < ITERS - 1:
            shapes = [slab] * (5 if stage == 1 else 6) + [slab, sums, sums]
            old_w = w
            results = call(kernel, f"step{stage}", shapes, operands, spectral)
            if stage == 1:
                z, w, r, q, t, f, keep, send = results
                s = old_w
            else:
                z, w, r, s, q, t, f, keep, send = results
        else:
            z, pay = call(kernel, f"step{stage}", [slab, (devices, SUB, LANE)], operands, spectral)
        basis.append(z)
    recv = exchange(pay)
    (potential_next,) = call(
        functools.partial(finish_kernel, sh), "finish", [slab], coefs + [recv, v_star] + basis
    )
    return potential_next, recovery_next


def solution(mesh):
    in_specs = (
        P(AXES, None, None),
        P(AXES, None, None),
        P(AXES, None, None),
        P("px", "py", None),
    )
    out_specs = (P(AXES, None, None), P(AXES, None, None))
    return jax.shard_map(local, mesh=mesh, in_specs=in_specs, out_specs=out_specs, check_vma=False)
```

```python
import functools
import math

import jax
import jax.numpy as jnp
import numpy as np
from jax import lax
from jax.experimental import pallas as pl
from jax.experimental.pallas import tpu as pltpu
from jax.sharding import PartitionSpec as P

ITERS = 4
mass_rate = 0.01
mean_conduct = 1.0
excite_gain = 8.0
threshold = 0.15
base_rate = 0.002
rate_slope = 0.2
rate_shift = 0.3
time_step = 0.1
alpha_low = 0.199
alpha_high = 5.03

AXES = ("px", "py")
SUB = 8
LANE = 128
VMEM = pltpu.MemorySpace.VMEM


def mode_order(length):
    return np.concatenate([np.arange(0, length, 2), np.arange(1, length, 2)])


def half_tables(length):
    points = np.arange(length // 2)
    tables = []
    for odd in range(2):
        modes = 2 * np.arange(length // 2) + odd
        angle = 2.0 * np.pi / length * (points[:, None] * modes[None, :] % length)
        tables.append(np.cos(angle) + np.sin(angle))
    return tables


def two_parts(table):
    high = table.astype(jnp.bfloat16)
    low = (table - high.astype(np.float64)).astype(jnp.bfloat16)
    return high, low, np.zeros_like(high)


def right_table(table):
    high, low, none = two_parts(table)
    return np.block([[high, low], [high, none]])


def left_table(table):
    high, low, none = two_parts(table)
    return np.block([[high, high], [low, none]])


def transform_tables(gy, gz):
    y_even, y_odd = half_tables(gy)
    z_even, z_odd = half_tables(gz)
    right = [right_table(z_even), right_table(z_odd), right_table(z_odd.T)]
    left = [left_table(y_even), left_table(y_odd.T), left_table(y_odd)]
    return np.stack(right + left)


forward_set = (0, 1, 3, 4)
backward_set = (0, 2, 3, 5)


def wave_term(length):
    return 2.0 - 2.0 * np.cos(2.0 * np.pi / length * np.arange(length))


def mode_tables(gx, gy, gz, planes):
    along_y = wave_term(gy)[mode_order(gy)]
    along_z = wave_term(gz)[mode_order(gz)]
    sigma = mass_rate / mean_conduct + along_y[:, None] + along_z[None, :]
    rho = 1.0 / (1.0 + 0.5 * sigma + np.sqrt(sigma + 0.25 * sigma * sigma))
    scale = rho / (1.0 - rho * rho) / (mean_conduct * gy * gz)
    block = rho**planes
    closure = 1.0 / (1.0 - rho**gx)
    return rho, scale, block, closure


def split_bf16(x):
    high = x.astype(jnp.bfloat16)
    low = (x - high.astype(jnp.float32)).astype(jnp.bfloat16)
    return high, low


def dot(a, b):
    return jnp.dot(a, b, preferred_element_type=jnp.float32)


def right_half(xh, xl, table):
    half = xh.shape[1]
    both = dot(jnp.concatenate([xh, xl], axis=1), table)
    return both[:, :half] + both[:, half:]


def left_half(x, table):
    half = x.shape[0]
    both = dot(table, jnp.concatenate(split_bf16(x), axis=0))
    return both[:half] + both[half:]


def forward_right(x, tables):
    half = x.shape[1] // 2
    a, b = x[:, :half], x[:, half:]
    even = right_half(*split_bf16(a + b), tables[0])
    odd = right_half(*split_bf16(a - b), tables[1])
    return jnp.concatenate([even, odd], axis=1)


def forward_left(x, tables):
    half = x.shape[0] // 2
    a, b = x[:half], x[half:]
    return left_half(a + b, tables[2]), left_half(a - b, tables[3])


def backward_right(xh, xl, tables):
    half = xh.shape[1] // 2
    even = right_half(xh[:, :half], xl[:, :half], tables[0])
    odd = right_half(xh[:, half:], xl[:, half:], tables[1])
    return jnp.concatenate([even + odd, even - odd], axis=1)


def backward_left(x, tables):
    half = x.shape[0] // 2
    even = left_half(x[:half], tables[2])
    odd = left_half(x[half:], tables[3])
    return even + odd, even - odd


def together(count):
    return max(k for k in range(1, 6) if count % k == 0)


class Shape:
    def __init__(self, planes, gy, gz, devices):
        self.planes, self.gy, self.gz, self.devices = planes, gy, gz, devices
        self.gx = planes * devices
        self.chips = devices // 2
        self.halves = gz // LANE
        self.per_group = 2 * self.halves
        self.groups = gy // SUB // 2
        self.tiles = self.groups * self.per_group
        self.slots = self.tiles // self.chips
        assert self.per_group % self.slots == 0
        self.rows = self.slots * SUB

    def tile(self, group, kind, half):
        return group * self.per_group + kind * self.halves + half

    def place(self, group, kind, half):
        q = kind * self.halves + half
        return group * (self.per_group // self.slots) + q // self.slots, q % self.slots * SUB


def emit_transform(source, js, tables, f_ref):
    right = [forward_right(source(j), tables) for j in js]
    for j, x in zip(js, right):
        top, low = forward_left(x, tables)
        half = top.shape[0]
        f_ref[j, :half] = top
        f_ref[j, half:] = low


def emit_transforms(source, start, count, table_ref, f_ref):
    tables = [table_ref[i] for i in forward_set]
    many = together(count)

    def several(i, _):
        emit_transform(source, [start + i * many + k for k in range(many)], tables, f_ref)
        return 0

    lax.fori_loop(0, count // many, several, 0)


def emit_sums(sh, core, rho, f_ref, keep_ref, send_ref, scal):
    for side, ref in ((core, keep_ref), (1 - core, send_ref)):

        def group(g, _, side=side, ref=ref):
            row = pl.multiple_of((side * sh.groups + g) * SUB, SUB)
            for half in range(sh.halves):
                lanes = slice(half * LANE, (half + 1) * LANE)
                decay = rho[pl.ds(row, SUB), lanes]
                f = [f_ref[j, pl.ds(row, SUB), lanes] for j in range(sh.planes)]
                p = f[0]
                e = f[-1]
                for j in range(1, sh.planes):
                    p = f[j] + decay * p
                    e = f[sh.planes - 1 - j] + decay * e
                ref[sh.tile(g, 0, half)] = p
                ref[sh.tile(g, 1, half)] = e
            return 0

        lax.fori_loop(0, sh.groups, group, 0, unroll=2)
        ref[sh.tiles] = scal


def join_kernel(sh, sums, core_ref, keep, other, block, out):
    core = core_ref[0]
    early = core == 0
    def group(g, _):
        row = pl.multiple_of((core * sh.groups + g) * SUB, SUB)
        for half in range(sh.halves):
            a = block[pl.ds(row, SUB), half * LANE : (half + 1) * LANE]
            for kind in range(2):
                at = sh.tile(g, kind, half)
                mine, its = keep[at], other[at]
                first = jnp.where(early, mine, its)
                second = jnp.where(early, its, mine)
                d, to = sh.place(g, kind, half)
                value = a * first + second if kind == 0 else first + a * second
                out[d, pl.ds(to, SUB), :] = value
        return 0

    lax.fori_loop(0, sh.groups, group, 0, unroll=4)

    if sums:
        scal = keep[sh.tiles] + other[sh.tiles]

        def spread(d, _):
            out[d, pl.ds(sh.rows, SUB), :] = scal
            return 0

        lax.fori_loop(0, sh.chips, spread, 0, unroll=4)


def part_kernel(sh, core_ref, carry, keep, other, block, own, send):
    core = core_ref[0]
    early = core == 0

    def group(g, _):
        row = pl.multiple_of((core * sh.groups + g) * SUB, SUB)
        for half in range(sh.halves):
            a = block[pl.ds(row, SUB), half * LANE : (half + 1) * LANE]
            for kind in range(2):
                at = sh.tile(g, kind, half)
                mine, its = keep[at], other[at]
                d, to = sh.place(g, kind, half)
                outer = carry[d, pl.ds(to, SUB), :]
                if kind == 0:
                    inner = jnp.where(early, mine, its) + a * outer
                    own[at] = jnp.where(early, outer, inner)
                    send[at] = jnp.where(early, inner, outer)
                else:
                    inner = jnp.where(early, its, mine) + a * outer
                    own[at] = jnp.where(early, inner, outer)
                    send[at] = jnp.where(early, outer, inner)
        return 0

    lax.fori_loop(0, sh.groups, group, 0, unroll=4)


def sideways(sh, j, here, gy_ref, gz_ref):
    flux = gy_ref[j] * (here - pltpu.roll(here, sh.gy - 1, 0))
    acc = flux - pltpu.roll(flux, 1, 0)
    flux = gz_ref[j] * (here - pltpu.roll(here, sh.gz - 1, 1))
    return acc + flux - pltpu.roll(flux, 1, 1)


def stencil(sh, j, here, before, after, gx_ref, gy_ref, gz_ref):
    acc = gx_ref[j + 1] * (here - after) - gx_ref[j] * (before - here)
    return acc + sideways(sh, j, here, gy_ref, gz_ref)


def fold(sh, x):
    return jnp.sum(x.reshape(sh.gy // SUB, SUB, sh.gz), axis=0)


def scal_tile(sh, parts):
    rows = []
    for part in parts:
        row = jnp.sum(part, axis=0, keepdims=True)
        total = row[:, :LANE]
        for half in range(1, sh.halves):
            total = total + row[:, half * LANE : (half + 1) * LANE]
        rows.append(total)
    rows.append(jnp.zeros((SUB - len(rows), LANE), jnp.float32))
    return jnp.concatenate(rows, axis=0)


def edge_kernel(sh, parts, place_ref, *refs):
    pieces, (first, last) = refs[:parts], refs[parts:]
    wide = sh.gy // parts
    for k in range(parts):
        at = pl.multiple_of((place_ref[0] ^ k) * wide, wide)
        first[0, pl.ds(at, wide), :] = pieces[k][0]
        last[0, pl.ds(at, wide), :] = pieces[k][1]


def start_kernel(sh, parts, place_ref, u, first, last, *refs):
    pieces = refs[: parts if sh.planes > 2 else 0]
    table_ref, gx, gy, gz, r, f, c = refs[len(pieces) :]
    wide = sh.gy // parts
    c[0] = 0.5 * first[0]
    c[sh.planes - 1] = 0.5 * last[0]
    for k, piece in enumerate(pieces):
        at = pl.multiple_of((place_ref[0] ^ k) * wide, wide)
        c[1 : sh.planes - 1, pl.ds(at, wide), :] = 0.5 * piece[...]

    def faces(j, _):
        own = c[j]
        gy[j] = own + pltpu.roll(own, sh.gy - 1, 0)
        gz[j] = own + pltpu.roll(own, sh.gz - 1, 1)
        return 0

    lax.fori_loop(0, sh.planes, faces, 0)
    def cross(j, _):
        gx[j] = c[j - 1] + c[j]
        return 0

    lax.fori_loop(1, sh.planes, cross, 0)

    end = sh.planes - 1
    r[0] = -(gx[1] * (u[0] - u[1]) + sideways(sh, 0, u[0], gy, gz))

    def inner(j, _):
        r[j] = -stencil(sh, j, u[j], u[j - 1], u[j + 1], gx, gy, gz)
        return 0

    lax.fori_loop(1, end, inner, 0)
    r[end] = -(gx[end] * (u[end] - u[end - 1]) + sideways(sh, end, u[end], gy, gz))
    if end > 1:
        emit_transforms(lambda j: r[j], 1, end - 1, table_ref, f)


def border_kernel(sh, core_ref, u, ulo, uhi, clo, chi, first, last, rho, table_ref, *refs):
    gx_in, r_in, _, gx, r, f, keep, send = refs
    end = sh.planes - 1
    low = 0.5 * (clo[0] + first[0])
    high = 0.5 * (chi[0] + last[0])
    gx[0] = low
    gx[sh.planes] = high
    r[0] = r_in[0] - low * (u[0] - ulo[0])
    r[end] = r_in[end] - high * (u[end] - uhi[0])
    emit_transform(lambda j: r[j], [0, end], [table_ref[i] for i in forward_set], f)
    emit_sums(sh, core_ref[0], rho, f, keep, send, jnp.zeros((SUB, LANE), jnp.float32))


def scan_kernel(sh, first, *refs):
    recv, decay, closure, onward = refs[:4]
    if first:
        (out,) = refs[4:]
    else:
        coef, out, coef_out = refs[4:]
    count = sh.chips

    def run(rows, forward, store):
        a = decay[rows]
        order = (lambda i: i) if forward else (lambda i: count - 1 - i)

        def total(i, s):
            return recv[order(i), rows, :] + a * s

        zero = jnp.zeros(a.shape, jnp.float32)
        carry = lax.fori_loop(0, count, total, zero, unroll=8) * closure[rows]

        def step(i, carry):
            store(order(i), carry)
            return recv[order(i), rows, :] + a * carry

        lax.fori_loop(0, count, step, carry, unroll=8)

    if sh.slots == sh.per_group:
        half = sh.rows // 2
        for rows, forward in ((slice(0, half), True), (slice(half, sh.rows), False)):

            def store(d, x, rows=rows):
                out[d, rows, :] = x

            run(rows, forward, store)
    else:
        rows = slice(0, sh.rows)
        take = onward[...]

        def store_forward(d, x):
            out[d] = x

        def store_backward(d, x):
            out[d] = jnp.where(take > 0.5, out[d], x)

        run(rows, True, store_forward)
        run(rows, False, store_backward)

    if not first:
        sums = sum_rows(sh.chips, recv, sh.rows)
        coef_out[...] = next_coefficients(sums, coef[...], sh.gz)


def sum_rows(count, recv, at):
    def add(d, s):
        return s + recv[d, at : at + SUB, :]

    return lax.fori_loop(1, count, add, recv[0, at : at + SUB, :], unroll=4)


def next_coefficients(sums, previous, width):
    product = jnp.maximum(jnp.sum(sums[0:1], axis=1, keepdims=True), 0.0)
    curve = jnp.sum(sums[1:2], axis=1, keepdims=True)
    product = jnp.broadcast_to(product, (1, width))
    curve = jnp.broadcast_to(curve, (1, width))
    old_product = previous[0:1]
    old_alpha = previous[1:2]
    started = old_product > 0.0
    beta = jnp.where(started, product / jnp.where(started, old_product, 1.0), 0.0)
    curve = curve - beta * product / jnp.where(old_alpha > 0.0, old_alpha, 1.0)
    usable = curve > 0.0
    alpha = jnp.where(usable, product / jnp.where(usable, curve, 1.0), alpha_low)
    alpha = jnp.clip(alpha, alpha_low, alpha_high)
    return jnp.concatenate(
        [product, alpha, beta, jnp.zeros((SUB - 3, width), jnp.float32)], axis=0
    )


def emit_inverse(sh, core, f, own, other, rho, scale, table_ref, uh, ul, m):
    tall = 2 * SUB
    for side, carry in ((core, own), (1 - core, other)):

        def group(i, _, side=side, carry=carry):
            row = pl.multiple_of(side * (sh.groups * SUB) + i * tall, tall)
            for half in range(sh.halves):
                lanes = slice(half * LANE, (half + 1) * LANE)
                decay = rho[pl.ds(row, tall), lanes]
                gain = scale[pl.ds(row, tall), lanes]
                first, final = (
                    jnp.concatenate(
                        [carry[sh.tile(g, kind, half)] for g in (2 * i, 2 * i + 1)], axis=0
                    )
                    for kind in range(2)
                )

                def put(j, value):
                    high, low = split_bf16(gain * value)
                    uh[j, pl.ds(row, tall), lanes] = high
                    ul[j, pl.ds(row, tall), lanes] = low

                fields = [f[j, pl.ds(row, tall), lanes] for j in range(sh.planes)]
                back = [None] * sh.planes
                e = final
                for j in reversed(range(sh.planes)):
                    back[j] = decay * e
                    e = fields[j] + back[j]
                put(0, first + decay * e)
                p = first
                for j in range(sh.planes):
                    p = fields[j] + decay * p
                    put(j + 1, p + back[j])
                put(sh.planes + 1, decay * p + final)
            return 0

        lax.fori_loop(0, sh.groups // 2, group, 0)
    tables = [table_ref[i] for i in backward_set]
    many = together(sh.planes + 2)

    def pair(i, _):
        js = [i * many + k for k in range(many)]
        right = [backward_right(uh[j], ul[j], tables) for j in js]
        for j, x in zip(js, right):
            top, low = backward_left(x, tables)
            m[j, : sh.gy // 2] = top
            m[j, sh.gy // 2 :] = low
        return 0

    lax.fori_loop(0, (sh.planes + 2) // many, pair, 0)


def step_kernel(sh, stage, *refs):
    names = ["core", "f", "own", "other", "rho", "scale", "tables", "gx", "gy", "gz", "r"]
    if stage > 0:
        names += ["coef", "z", "w"]
    if stage > 1:
        names += ["s", "q", "t"]
    last = stage == ITERS - 1
    if stage == 0:
        outs = ["z_new", "w_new"]
    elif last:
        outs = ["z_new"]
    else:
        outs = ["z_new", "w_new", "r_new", "s_new", "q_new", "t_new"]
        if stage == 1:
            outs.remove("s_new")
    outs += ["pay"] if last else ["f_new", "keep", "send"]
    scratch = ["uh", "ul", "m"]
    k = dict(zip(names + outs + scratch, refs, strict=True))
    m = k["m"]
    core = k["core"][0]
    tables = (k["rho"], k["scale"], k["tables"])
    emit_inverse(sh, core, k["f"], k["own"], k["other"], *tables, k["uh"], k["ul"], m)
    if stage > 0:
        alpha = k["coef"][1:2, :]
        beta = k["coef"][2:3, :]

    def plane(j, sums):
        here = m[j + 1]
        image = mass_rate * here + mean_conduct * stencil(
            sh, j, here, m[j], m[j + 2], k["gx"], k["gy"], k["gz"]
        )
        if stage == 0:
            z, w, r = here, image, k["r"][j]
        else:
            s, q, t = k["w"][j], here, image
            if stage > 1:
                s = s + beta * k["s"][j]
                q = q + beta * k["q"][j]
                t = t + beta * k["t"][j]
            r = k["r"][j] - alpha * s
            z = k["z"][j] - alpha * q
            w = k["w"][j] - alpha * t
            if not last:
                k["r_new"][j] = r
                k["q_new"][j] = q
                k["t_new"][j] = t
                if stage > 1:
                    k["s_new"][j] = s
        k["z_new"][j] = z
        if not last:
            k["w_new"][j] = w
        return (sums[0] + fold(sh, r * z), sums[1] + fold(sh, w * z))

    zero = jnp.zeros((SUB, sh.gz), jnp.float32)
    scal = scal_tile(sh, lax.fori_loop(0, sh.planes, plane, (zero, zero)))
    if last:
        pay = k["pay"]

        def spread(d, _):
            pay[d] = scal
            return 0

        lax.fori_loop(0, sh.devices, spread, 0)
    else:
        w_new = k["w_new"]
        into = (k["f_new"], k["keep"], k["send"])
        emit_transforms(lambda j: w_new[j], 0, sh.planes, k["tables"], k["f_new"])
        emit_sums(sh, core, k["rho"], *into, scal)


def finish_kernel(sh, *refs):
    coefs = refs[: ITERS - 1]
    recv = refs[ITERS - 1]
    u = refs[ITERS]
    fields = refs[ITERS + 1 : 2 * ITERS + 1]
    out = refs[-1]
    rows = [c[...] for c in coefs]
    rows.append(next_coefficients(sum_rows(sh.devices, recv, 0), rows[-1], sh.gz))
    weight = rows[-1][1:2]
    weights = [weight]
    for i in reversed(range(ITERS - 1)):
        weight = rows[i][1:2] + rows[i + 1][2:3] * weight
        weights.insert(0, weight)

    def plane(j, _):
        total = u[j]
        for weight, field in zip(weights, fields):
            total = total + weight * field[j]
        out[j] = total
        return 0

    lax.fori_loop(0, sh.planes, plane, 0)


def call(kernel, name, out_shapes, operands, scratch=(), aliases=None):
    whole = pl.BlockSpec(memory_space=VMEM)
    return pl.pallas_call(
        kernel,
        name=name,
        out_shape=[jax.ShapeDtypeStruct(s, jnp.float32) for s in out_shapes],
        in_specs=[
            pl.BlockSpec(memory_space=pltpu.MemorySpace.SMEM) if x.dtype == jnp.int32 else whole
            for x in operands
        ],
        out_specs=[whole] * len(out_shapes),
        scratch_shapes=list(scratch),
        input_output_aliases=aliases or {},
        compiler_params=pltpu.CompilerParams(vmem_limit_bytes=12 * 1024 * 1024),
    )(*operands)


def exchange(x, groups=None):
    return lax.all_to_all(
        x, AXES, split_axis=0, concat_axis=0, tiled=True, axis_index_groups=groups
    )


def neighbours(first, final, axes):
    count = lax.axis_size(axes)
    return (
        lax.ppermute(final, axes, [(i, (i + 1) % count) for i in range(count)]),
        lax.ppermute(first, axes, [((i + 1) % count, i) for i in range(count)]),
    )


def local(potential, recovery, stimulus, conductivity):
    parts = lax.axis_size("py")
    devices = lax.axis_size("px") * parts
    planes, gy, gz = potential.shape
    sh = Shape(planes, gy, gz, devices)

    rho, scale, block, closure = mode_tables(sh.gx, gy, gz, planes)
    groups = gy // SUB

    def own_tiles(table):
        tiles = table.astype(np.float32).reshape(groups, SUB, sh.halves, LANE).transpose(0, 2, 1, 3)
        both = np.concatenate([tiles, tiles], axis=1).reshape(2, sh.chips, sh.rows, LANE)
        both = both.transpose(1, 0, 2, 3).reshape(devices, sh.rows, LANE)
        return lax.dynamic_index_in_dim(jnp.asarray(both), lax.axis_index(AXES), 0, False)

    across = jnp.asarray(block.astype(np.float32))
    block = own_tiles(block * block)
    closure = own_tiles(closure)
    core = jnp.reshape(lax.axis_index(AXES) % 2, (1,))
    place = jnp.reshape(lax.axis_index("py"), (1,))
    slot = lax.axis_index(AXES) // 2 * sh.slots + jnp.arange(sh.rows, dtype=jnp.int32)[:, None] // SUB
    onward = jnp.broadcast_to(
        (slot % sh.per_group < sh.halves).astype(jnp.float32), (sh.rows, LANE)
    )
    rho = jnp.asarray(rho.astype(np.float32))
    scale = jnp.asarray(scale.astype(np.float32))
    tables = jnp.asarray(transform_tables(gy, gz))

    coef = jnp.zeros((SUB, gz), jnp.float32)
    conductivity, block, closure, onward, coef, core = lax.optimization_barrier(
        (conductivity, block, closure, onward, coef, core)
    )
    wide = conductivity.shape[1]
    blocks = conductivity.reshape(parts, planes, wide, gz)
    mine = lax.axis_index("py")
    pieces = [lax.dynamic_index_in_dim(blocks, mine ^ k, 0, False) for k in range(parts)]
    edges = [jnp.stack([x[0], x[planes - 1]]) for x in pieces]
    inner = [x[1 : planes - 1] for x in pieces] if planes > 2 else []

    def across_y(items):
        return [
            lax.ppermute(x, "py", [(i, i ^ k) for i in range(parts)]) if k else x
            for k, x in enumerate(items)
        ]

    edges = across_y(edges)
    inner = across_y(inner)
    drive = (
        excite_gain * potential * (potential - threshold) * (1.0 - potential) - potential * recovery
    )
    v_star = potential + time_step * (drive + stimulus)
    rate = base_rate + rate_slope * recovery / (potential + rate_shift)
    recovery_next = recovery + time_step * rate * (
        -recovery - excite_gain * potential * (potential - threshold - 1.0)
    )
    ulo, uhi = neighbours(v_star[:1], v_star[-1:], AXES)

    slab = (planes, gy, gz)
    payload = (sh.chips, sh.rows + SUB, LANE)
    carries = (sh.chips, sh.rows, LANE)
    sums = (sh.tiles + 1, SUB, LANE)
    parted = (sh.tiles, SUB, LANE)
    swap = [(i, i ^ 1) for i in range(devices)]
    same_core = [[2 * chip + side for chip in range(sh.chips)] for side in range(2)]
    plane = (1, gy, gz)
    first, last = call(
        functools.partial(edge_kernel, sh, parts), "edges", [plane, plane], [place] + edges
    )
    clo, chi = neighbours(first, last, AXES)
    gxf, gyf, gzf, r, f = call(
        functools.partial(start_kernel, sh, parts),
        "start",
        [(planes + 1, gy, gz), slab, slab, slab, slab],
        [place, v_star, first, last] + inner + [tables],
        [pltpu.VMEM(slab, jnp.float32)],
    )
    operands = [core, v_star, ulo, uhi, clo, chi, first, last, rho, tables, gxf, r, f]
    gxf, r, f, keep, send = call(
        functools.partial(border_kernel, sh),
        "border",
        [(planes + 1, gy, gz), slab, slab, sums, sums],
        operands,
        aliases={10: 0, 11: 1, 12: 2},
    )
    spectral = [
        pltpu.VMEM((planes + 2, gy, gz), jnp.bfloat16),
        pltpu.VMEM((planes + 2, gy, gz), jnp.bfloat16),
        pltpu.VMEM((planes + 2, gy, gz), jnp.float32),
    ]
    coefs = []
    basis = []
    z = w = s = q = t = None
    for stage in range(ITERS):
        other = lax.ppermute(send, AXES, swap)
        (pay,) = call(
            functools.partial(join_kernel, sh, stage > 0),
            f"join{stage}",
            [payload if stage > 0 else carries],
            [core, keep, other, across],
        )
        recv = exchange(pay, same_core)
        if stage == 0:
            (carry,) = call(
                functools.partial(scan_kernel, sh, True),
                "scan0",
                [carries],
                [recv, block, closure, onward],
            )
        else:
            carry, coef = call(
                functools.partial(scan_kernel, sh, False),
                f"scan{stage}",
                [carries, (SUB, gz)],
                [recv, block, closure, onward, coef],
            )
            coefs.append(coef)
        carry = exchange(carry, same_core)
        own, send = call(
            functools.partial(part_kernel, sh),
            f"part{stage}",
            [parted, parted],
            [core, carry, keep, other, across],
        )
        other = lax.ppermute(send, AXES, swap)
        operands = [core, f, own, other, rho, scale, tables, gxf, gyf, gzf, r]
        if stage > 0:
            operands += [coef, z, w]
        if stage > 1:
            operands += [s, q, t]
        kernel = functools.partial(step_kernel, sh, stage)
        if stage == 0:
            shapes = [slab, slab, slab, sums, sums]
            z, w, f, keep, send = call(kernel, "step0", shapes, operands, spectral)
        elif stage < ITERS - 1:
            shapes = [slab] * (5 if stage == 1 else 6) + [slab, sums, sums]
            old_w = w
            results = call(kernel, f"step{stage}", shapes, operands, spectral)
            if stage == 1:
                z, w, r, q, t, f, keep, send = results
                s = old_w
            else:
                z, w, r, s, q, t, f, keep, send = results
        else:
            z, pay = call(kernel, f"step{stage}", [slab, (devices, SUB, LANE)], operands, spectral)
        basis.append(z)
    recv = exchange(pay)
    (potential_next,) = call(
        functools.partial(finish_kernel, sh), "finish", [slab], coefs + [recv, v_star] + basis
    )
    return potential_next, recovery_next


def solution(mesh):
    in_specs = (
        P(AXES, None, None),
        P(AXES, None, None),
        P(AXES, None, None),
        P("px", "py", None),
    )
    out_specs = (P(AXES, None, None), P(AXES, None, None))
    return jax.shard_map(local, mesh=mesh, in_specs=in_specs, out_specs=out_specs, check_vma=False)
```

```python
import functools
import math

import jax
import jax.numpy as jnp
import numpy as np
from jax import lax
from jax.experimental import pallas as pl
from jax.experimental.pallas import tpu as pltpu
from jax.sharding import PartitionSpec as P

ITERS = 4
mass_rate = 0.01
mean_conduct = 1.0
excite_gain = 8.0
threshold = 0.15
base_rate = 0.002
rate_slope = 0.2
rate_shift = 0.3
time_step = 0.1
alpha_low = 0.199
alpha_high = 5.03

AXES = ("px", "py")
SUB = 8
LANE = 128
VMEM = pltpu.MemorySpace.VMEM


def mode_order(length):
    return np.concatenate([np.arange(0, length, 2), np.arange(1, length, 2)])


def half_tables(length):
    points = np.arange(length // 2)
    tables = []
    for odd in range(2):
        modes = 2 * np.arange(length // 2) + odd
        angle = 2.0 * np.pi / length * (points[:, None] * modes[None, :] % length)
        tables.append(np.cos(angle) + np.sin(angle))
    return tables


def two_parts(table):
    high = table.astype(jnp.bfloat16)
    low = (table - high.astype(np.float64)).astype(jnp.bfloat16)
    return high, low, np.zeros_like(high)


def right_table(table):
    high, low, none = two_parts(table)
    return np.block([[high, low], [high, none]])


def left_table(table):
    high, low, none = two_parts(table)
    return np.block([[high, high], [low, none]])


def transform_tables(gy, gz):
    y_even, y_odd = half_tables(gy)
    z_even, z_odd = half_tables(gz)
    right = [right_table(z_even), right_table(z_odd), right_table(z_odd.T)]
    left = [left_table(y_even), left_table(y_odd.T), left_table(y_odd)]
    return np.stack(right + left)


forward_set = (0, 1, 3, 4)
backward_set = (0, 2, 3, 5)


def wave_term(length):
    return 2.0 - 2.0 * np.cos(2.0 * np.pi / length * np.arange(length))


def mode_tables(gx, gy, gz, planes):
    along_y = wave_term(gy)[mode_order(gy)]
    along_z = wave_term(gz)[mode_order(gz)]
    sigma = mass_rate / mean_conduct + along_y[:, None] + along_z[None, :]
    rho = 1.0 / (1.0 + 0.5 * sigma + np.sqrt(sigma + 0.25 * sigma * sigma))
    scale = rho / (1.0 - rho * rho) / (mean_conduct * gy * gz)
    block = rho**planes
    closure = 1.0 / (1.0 - rho**gx)
    return rho, scale, block, closure


def split_bf16(x):
    high = x.astype(jnp.bfloat16)
    low = (x - high.astype(jnp.float32)).astype(jnp.bfloat16)
    return high, low


def dot(a, b):
    return jnp.dot(a, b, preferred_element_type=jnp.float32)


def right_half(xh, xl, table):
    half = xh.shape[1]
    both = dot(jnp.concatenate([xh, xl], axis=1), table)
    return both[:, :half] + both[:, half:]


def left_half(x, table):
    half = x.shape[0]
    both = dot(table, jnp.concatenate(split_bf16(x), axis=0))
    return both[:half] + both[half:]


def forward_right(x, tables):
    half = x.shape[1] // 2
    a, b = x[:, :half], x[:, half:]
    even = right_half(*split_bf16(a + b), tables[0])
    odd = right_half(*split_bf16(a - b), tables[1])
    return jnp.concatenate([even, odd], axis=1)


def forward_left(x, tables):
    half = x.shape[0] // 2
    a, b = x[:half], x[half:]
    return left_half(a + b, tables[2]), left_half(a - b, tables[3])


def backward_right(xh, xl, tables):
    half = xh.shape[1] // 2
    even = right_half(xh[:, :half], xl[:, :half], tables[0])
    odd = right_half(xh[:, half:], xl[:, half:], tables[1])
    return jnp.concatenate([even + odd, even - odd], axis=1)


def backward_left(x, tables):
    half = x.shape[0] // 2
    even = left_half(x[:half], tables[2])
    odd = left_half(x[half:], tables[3])
    return even + odd, even - odd


def together(count):
    return max(k for k in range(1, 6) if count % k == 0)


class Shape:
    def __init__(self, planes, gy, gz, devices):
        self.planes, self.gy, self.gz, self.devices = planes, gy, gz, devices
        self.gx = planes * devices
        self.chips = devices // 2
        self.halves = gz // LANE
        self.per_group = 2 * self.halves
        self.groups = gy // SUB // 2
        self.tiles = self.groups * self.per_group
        self.slots = self.tiles // self.chips
        assert self.per_group % self.slots == 0
        self.rows = self.slots * SUB

    def tile(self, group, kind, half):
        return group * self.per_group + kind * self.halves + half

    def place(self, group, kind, half):
        q = kind * self.halves + half
        return group * (self.per_group // self.slots) + q // self.slots, q % self.slots * SUB


def emit_transform(source, js, tables, f_ref):
    right = [forward_right(source(j), tables) for j in js]
    for j, x in zip(js, right):
        top, low = forward_left(x, tables)
        half = top.shape[0]
        f_ref[j, :half] = top
        f_ref[j, half:] = low


def emit_transforms(source, start, count, table_ref, f_ref):
    tables = [table_ref[i] for i in forward_set]
    many = together(count)

    def several(i, _):
        emit_transform(source, [start + i * many + k for k in range(many)], tables, f_ref)
        return 0

    lax.fori_loop(0, count // many, several, 0)


def emit_sums(sh, core, rho, f_ref, keep_ref, send_ref, scal):
    for side, ref in ((core, keep_ref), (1 - core, send_ref)):

        def group(g, _, side=side, ref=ref):
            row = pl.multiple_of((side * sh.groups + g) * SUB, SUB)
            for half in range(sh.halves):
                lanes = slice(half * LANE, (half + 1) * LANE)
                decay = rho[pl.ds(row, SUB), lanes]
                f = [f_ref[j, pl.ds(row, SUB), lanes] for j in range(sh.planes)]
                p = f[0]
                e = f[-1]
                for j in range(1, sh.planes):
                    p = f[j] + decay * p
                    e = f[sh.planes - 1 - j] + decay * e
                ref[sh.tile(g, 0, half)] = p
                ref[sh.tile(g, 1, half)] = e
            return 0

        lax.fori_loop(0, sh.groups, group, 0, unroll=2)
        ref[sh.tiles] = scal


def join_kernel(sh, sums, core_ref, keep, other, block, out):
    core = core_ref[0]
    early = core == 0
    def group(g, _):
        row = pl.multiple_of((core * sh.groups + g) * SUB, SUB)
        for half in range(sh.halves):
            a = block[pl.ds(row, SUB), half * LANE : (half + 1) * LANE]
            for kind in range(2):
                at = sh.tile(g, kind, half)
                mine, its = keep[at], other[at]
                first = jnp.where(early, mine, its)
                second = jnp.where(early, its, mine)
                d, to = sh.place(g, kind, half)
                value = a * first + second if kind == 0 else first + a * second
                out[d, pl.ds(to, SUB), :] = value
        return 0

    lax.fori_loop(0, sh.groups, group, 0, unroll=4)

    if sums:
        scal = keep[sh.tiles] + other[sh.tiles]

        def spread(d, _):
            out[d, pl.ds(sh.rows, SUB), :] = scal
            return 0

        lax.fori_loop(0, sh.chips, spread, 0, unroll=4)


def part_kernel(sh, core_ref, carry, keep, other, block, own, send):
    core = core_ref[0]
    early = core == 0

    def group(g, _):
        row = pl.multiple_of((core * sh.groups + g) * SUB, SUB)
        for half in range(sh.halves):
            a = block[pl.ds(row, SUB), half * LANE : (half + 1) * LANE]
            for kind in range(2):
                at = sh.tile(g, kind, half)
                mine, its = keep[at], other[at]
                d, to = sh.place(g, kind, half)
                outer = carry[d, pl.ds(to, SUB), :]
                if kind == 0:
                    inner = jnp.where(early, mine, its) + a * outer
                    own[at] = jnp.where(early, outer, inner)
                    send[at] = jnp.where(early, inner, outer)
                else:
                    inner = jnp.where(early, its, mine) + a * outer
                    own[at] = jnp.where(early, inner, outer)
                    send[at] = jnp.where(early, outer, inner)
        return 0

    lax.fori_loop(0, sh.groups, group, 0, unroll=4)


def sideways(sh, j, here, gy_ref, gz_ref):
    flux = gy_ref[j] * (here - pltpu.roll(here, sh.gy - 1, 0))
    acc = flux - pltpu.roll(flux, 1, 0)
    flux = gz_ref[j] * (here - pltpu.roll(here, sh.gz - 1, 1))
    return acc + flux - pltpu.roll(flux, 1, 1)


def stencil(sh, j, here, before, after, gx_ref, gy_ref, gz_ref):
    acc = gx_ref[j + 1] * (here - after) - gx_ref[j] * (before - here)
    return acc + sideways(sh, j, here, gy_ref, gz_ref)


def fold(sh, x):
    return jnp.sum(x.reshape(sh.gy // SUB, SUB, sh.gz), axis=0)


def scal_tile(sh, parts):
    rows = []
    for part in parts:
        row = jnp.sum(part, axis=0, keepdims=True)
        total = row[:, :LANE]
        for half in range(1, sh.halves):
            total = total + row[:, half * LANE : (half + 1) * LANE]
        rows.append(total)
    rows.append(jnp.zeros((SUB - len(rows), LANE), jnp.float32))
    return jnp.concatenate(rows, axis=0)


def edge_kernel(sh, parts, place_ref, *refs):
    pieces, (first, last) = refs[:parts], refs[parts:]
    wide = sh.gy // parts
    for k in range(parts):
        at = pl.multiple_of((place_ref[0] ^ k) * wide, wide)
        first[0, pl.ds(at, wide), :] = pieces[k][0]
        last[0, pl.ds(at, wide), :] = pieces[k][1]


def start_kernel(sh, parts, place_ref, u, first, last, *refs):
    pieces = refs[: parts if sh.planes > 2 else 0]
    table_ref, gx, gy, gz, r, f, c = refs[len(pieces) :]
    wide = sh.gy // parts
    c[0] = 0.5 * first[0]
    c[sh.planes - 1] = 0.5 * last[0]
    for k, piece in enumerate(pieces):
        at = pl.multiple_of((place_ref[0] ^ k) * wide, wide)
        c[1 : sh.planes - 1, pl.ds(at, wide), :] = 0.5 * piece[...]

    def faces(j, _):
        own = c[j]
        gy[j] = own + pltpu.roll(own, sh.gy - 1, 0)
        gz[j] = own + pltpu.roll(own, sh.gz - 1, 1)
        return 0

    lax.fori_loop(0, sh.planes, faces, 0)
    def cross(j, _):
        gx[j] = c[j - 1] + c[j]
        return 0

    lax.fori_loop(1, sh.planes, cross, 0)

    end = sh.planes - 1
    r[0] = -(gx[1] * (u[0] - u[1]) + sideways(sh, 0, u[0], gy, gz))

    def inner(j, _):
        r[j] = -stencil(sh, j, u[j], u[j - 1], u[j + 1], gx, gy, gz)
        return 0

    lax.fori_loop(1, end, inner, 0)
    r[end] = -(gx[end] * (u[end] - u[end - 1]) + sideways(sh, end, u[end], gy, gz))
    if end > 1:
        emit_transforms(lambda j: r[j], 1, end - 1, table_ref, f)


def border_kernel(sh, core_ref, u, ulo, uhi, clo, chi, first, last, rho, table_ref, *refs):
    gx_in, r_in, _, gx, r, f, keep, send = refs
    end = sh.planes - 1
    low = 0.5 * (clo[0] + first[0])
    high = 0.5 * (chi[0] + last[0])
    gx[0] = low
    gx[sh.planes] = high
    r[0] = r_in[0] - low * (u[0] - ulo[0])
    r[end] = r_in[end] - high * (u[end] - uhi[0])
    emit_transform(lambda j: r[j], [0, end], [table_ref[i] for i in forward_set], f)
    emit_sums(sh, core_ref[0], rho, f, keep, send, jnp.zeros((SUB, LANE), jnp.float32))


def scan_kernel(sh, first, *refs):
    recv, decay, closure, onward = refs[:4]
    if first:
        (out,) = refs[4:]
    else:
        coef, out, coef_out = refs[4:]
    count = sh.chips

    def run(rows, forward, store):
        a = decay[rows]
        order = (lambda i: i) if forward else (lambda i: count - 1 - i)

        def total(i, s):
            return recv[order(i), rows, :] + a * s

        zero = jnp.zeros(a.shape, jnp.float32)
        carry = lax.fori_loop(0, count, total, zero, unroll=8) * closure[rows]

        def step(i, carry):
            store(order(i), carry)
            return recv[order(i), rows, :] + a * carry

        lax.fori_loop(0, count, step, carry, unroll=8)

    if sh.slots == sh.per_group:
        half = sh.rows // 2
        for rows, forward in ((slice(0, half), True), (slice(half, sh.rows), False)):

            def store(d, x, rows=rows):
                out[d, rows, :] = x

            run(rows, forward, store)
    else:
        rows = slice(0, sh.rows)
        take = onward[...]

        def store_forward(d, x):
            out[d] = x

        def store_backward(d, x):
            out[d] = jnp.where(take > 0.5, out[d], x)

        run(rows, True, store_forward)
        run(rows, False, store_backward)

    if not first:
        sums = sum_rows(sh.chips, recv, sh.rows)
        coef_out[...] = next_coefficients(sums, coef[...], sh.gz)


def sum_rows(count, recv, at):
    def add(d, s):
        return s + recv[d, at : at + SUB, :]

    return lax.fori_loop(1, count, add, recv[0, at : at + SUB, :], unroll=4)


def next_coefficients(sums, previous, width):
    product = jnp.maximum(jnp.sum(sums[0:1], axis=1, keepdims=True), 0.0)
    curve = jnp.sum(sums[1:2], axis=1, keepdims=True)
    product = jnp.broadcast_to(product, (1, width))
    curve = jnp.broadcast_to(curve, (1, width))
    old_product = previous[0:1]
    old_alpha = previous[1:2]
    started = old_product > 0.0
    beta = jnp.where(started, product / jnp.where(started, old_product, 1.0), 0.0)
    curve = curve - beta * product / jnp.where(old_alpha > 0.0, old_alpha, 1.0)
    usable = curve > 0.0
    alpha = jnp.where(usable, product / jnp.where(usable, curve, 1.0), alpha_low)
    alpha = jnp.clip(alpha, alpha_low, alpha_high)
    return jnp.concatenate(
        [product, alpha, beta, jnp.zeros((SUB - 3, width), jnp.float32)], axis=0
    )


def emit_inverse(sh, core, f, own, other, rho, scale, table_ref, uh, ul, m):
    tall = 2 * SUB
    for side, carry in ((core, own), (1 - core, other)):

        def group(i, _, side=side, carry=carry):
            row = pl.multiple_of(side * (sh.groups * SUB) + i * tall, tall)
            for half in range(sh.halves):
                lanes = slice(half * LANE, (half + 1) * LANE)
                decay = rho[pl.ds(row, tall), lanes]
                gain = scale[pl.ds(row, tall), lanes]
                first, final = (
                    jnp.concatenate(
                        [carry[sh.tile(g, kind, half)] for g in (2 * i, 2 * i + 1)], axis=0
                    )
                    for kind in range(2)
                )

                def put(j, value):
                    high, low = split_bf16(gain * value)
                    uh[j, pl.ds(row, tall), lanes] = high
                    ul[j, pl.ds(row, tall), lanes] = low

                fields = [f[j, pl.ds(row, tall), lanes] for j in range(sh.planes)]
                back = [None] * sh.planes
                e = final
                for j in reversed(range(sh.planes)):
                    back[j] = decay * e
                    e = fields[j] + back[j]
                put(0, first + decay * e)
                p = first
                for j in range(sh.planes):
                    p = fields[j] + decay * p
                    put(j + 1, p + back[j])
                put(sh.planes + 1, decay * p + final)
            return 0

        lax.fori_loop(0, sh.groups // 2, group, 0)
    tables = [table_ref[i] for i in backward_set]
    many = together(sh.planes + 2)

    def pair(i, _):
        js = [i * many + k for k in range(many)]
        right = [backward_right(uh[j], ul[j], tables) for j in js]
        for j, x in zip(js, right):
            top, low = backward_left(x, tables)
            m[j, : sh.gy // 2] = top
            m[j, sh.gy // 2 :] = low
        return 0

    lax.fori_loop(0, (sh.planes + 2) // many, pair, 0)


def step_kernel(sh, stage, *refs):
    names = ["core", "f", "own", "other", "rho", "scale", "tables", "gx", "gy", "gz", "r"]
    if stage > 0:
        names += ["coef", "z", "w"]
    if stage > 1:
        names += ["s", "q", "t"]
    last = stage == ITERS - 1
    if stage == 0:
        outs = ["z_new", "w_new"]
    elif last:
        outs = ["z_new"]
    else:
        outs = ["z_new", "w_new", "r_new", "s_new", "q_new", "t_new"]
        if stage == 1:
            outs.remove("s_new")
    outs += ["pay"] if last else ["f_new", "keep", "send"]
    scratch = ["uh", "ul", "m"]
    k = dict(zip(names + outs + scratch, refs, strict=True))
    m = k["m"]
    core = k["core"][0]
    tables = (k["rho"], k["scale"], k["tables"])
    emit_inverse(sh, core, k["f"], k["own"], k["other"], *tables, k["uh"], k["ul"], m)
    if stage > 0:
        alpha = k["coef"][1:2, :]
        beta = k["coef"][2:3, :]

    def plane(j, sums):
        here = m[j + 1]
        image = mass_rate * here + mean_conduct * stencil(
            sh, j, here, m[j], m[j + 2], k["gx"], k["gy"], k["gz"]
        )
        if stage == 0:
            z, w, r = here, image, k["r"][j]
        else:
            s, q, t = k["w"][j], here, image
            if stage > 1:
                s = s + beta * k["s"][j]
                q = q + beta * k["q"][j]
                t = t + beta * k["t"][j]
            r = k["r"][j] - alpha * s
            z = k["z"][j] - alpha * q
            w = k["w"][j] - alpha * t
            if not last:
                k["r_new"][j] = r
                k["q_new"][j] = q
                k["t_new"][j] = t
                if stage > 1:
                    k["s_new"][j] = s
        k["z_new"][j] = z
        if not last:
            k["w_new"][j] = w
        return (sums[0] + fold(sh, r * z), sums[1] + fold(sh, w * z))

    zero = jnp.zeros((SUB, sh.gz), jnp.float32)
    scal = scal_tile(sh, lax.fori_loop(0, sh.planes, plane, (zero, zero)))
    if last:
        pay = k["pay"]
        lane = lax.broadcasted_iota(jnp.int32, (1, LANE), 1)
        folded = scal + pltpu.roll(scal, LANE // 2, 1)
        row = jnp.where(lane < LANE // 2, folded[0:1], folded[1:2])

        def spread(d, _):
            pay[d] = row
            return 0

        lax.fori_loop(0, sh.devices, spread, 0)
    else:
        w_new = k["w_new"]
        into = (k["f_new"], k["keep"], k["send"])
        emit_transforms(lambda j: w_new[j], 0, sh.planes, k["tables"], k["f_new"])
        emit_sums(sh, core, k["rho"], *into, scal)


def blend_kernel(sh, *refs):
    count = ITERS - 1
    rows = [c[...] for c in refs[:count]]
    u = refs[count]
    fields = refs[count + 1 : 2 * count + 1]
    total, direction = refs[2 * count + 1 :]
    weight = rows[-1][1:2]
    weights = [weight]
    for i in reversed(range(count - 1)):
        weight = rows[i][1:2] + rows[i + 1][2:3] * weight
        weights.insert(0, weight)

    def plane(j, _):
        value = u[j]
        along = jnp.zeros_like(value)
        for weight, row, field in zip(weights, rows, fields):
            basis = field[j]
            value = value + weight * basis
            along = basis + row[2:3] * along
        total[j] = value
        direction[j] = along
        return 0

    lax.fori_loop(0, sh.planes, plane, 0)


def finish_kernel(sh, coef, recv, before, direction, last, out, total, done):
    row = jnp.sum(recv[...], axis=0)
    first = lax.broadcasted_iota(jnp.int32, row.shape, 1) < LANE // 2
    none = jnp.zeros_like(row)
    both = jnp.concatenate([jnp.where(first, row, none), jnp.where(first, none, row)], axis=0)
    row = next_coefficients(both, coef[...], sh.gz)
    alpha, beta = row[1:2], row[2:3]

    def copy(j):
        return pltpu.make_async_copy(total.at[j], out.at[j], done.at[j])

    for j in range(sh.planes):
        total[j] = before[j] + alpha * (last[j] + beta * direction[j])
        copy(j).start()
    for j in range(sh.planes):
        copy(j).wait()


def call(kernel, name, out_shapes, operands, scratch=(), aliases=None, out_space=VMEM):
    whole = pl.BlockSpec(memory_space=VMEM)
    return pl.pallas_call(
        kernel,
        name=name,
        out_shape=[jax.ShapeDtypeStruct(s, jnp.float32) for s in out_shapes],
        in_specs=[
            pl.BlockSpec(memory_space=pltpu.MemorySpace.SMEM) if x.dtype == jnp.int32 else whole
            for x in operands
        ],
        out_specs=[pl.BlockSpec(memory_space=out_space)] * len(out_shapes),
        scratch_shapes=list(scratch),
        input_output_aliases=aliases or {},
        compiler_params=pltpu.CompilerParams(vmem_limit_bytes=12 * 1024 * 1024),
    )(*operands)


def exchange(x, groups=None):
    return lax.all_to_all(
        x, AXES, split_axis=0, concat_axis=0, tiled=True, axis_index_groups=groups
    )


def neighbours(first, final, axes):
    count = lax.axis_size(axes)
    return (
        lax.ppermute(final, axes, [(i, (i + 1) % count) for i in range(count)]),
        lax.ppermute(first, axes, [((i + 1) % count, i) for i in range(count)]),
    )


def local(potential, recovery, stimulus, conductivity):
    parts = lax.axis_size("py")
    devices = lax.axis_size("px") * parts
    planes, gy, gz = potential.shape
    sh = Shape(planes, gy, gz, devices)

    rho, scale, block, closure = mode_tables(sh.gx, gy, gz, planes)
    groups = gy // SUB

    def own_tiles(table):
        tiles = table.astype(np.float32).reshape(groups, SUB, sh.halves, LANE).transpose(0, 2, 1, 3)
        both = np.concatenate([tiles, tiles], axis=1).reshape(2, sh.chips, sh.rows, LANE)
        both = both.transpose(1, 0, 2, 3).reshape(devices, sh.rows, LANE)
        return lax.dynamic_index_in_dim(jnp.asarray(both), lax.axis_index(AXES), 0, False)

    across = jnp.asarray(block.astype(np.float32))
    block = own_tiles(block * block)
    closure = own_tiles(closure)
    core = jnp.reshape(lax.axis_index(AXES) % 2, (1,))
    place = jnp.reshape(lax.axis_index("py"), (1,))
    slot = lax.axis_index(AXES) // 2 * sh.slots + jnp.arange(sh.rows, dtype=jnp.int32)[:, None] // SUB
    onward = jnp.broadcast_to(
        (slot % sh.per_group < sh.halves).astype(jnp.float32), (sh.rows, LANE)
    )
    rho = jnp.asarray(rho.astype(np.float32))
    scale = jnp.asarray(scale.astype(np.float32))
    tables = jnp.asarray(transform_tables(gy, gz))

    coef = jnp.zeros((SUB, gz), jnp.float32)
    potential, block, closure, onward, coef, core = lax.optimization_barrier(
        (potential, block, closure, onward, coef, core)
    )
    wide = conductivity.shape[1]
    blocks = conductivity.reshape(parts, planes, wide, gz)
    mine = lax.axis_index("py")
    pieces = [lax.dynamic_index_in_dim(blocks, mine ^ k, 0, False) for k in range(parts)]
    edges = [jnp.stack([x[0], x[planes - 1]]) for x in pieces]
    inner = [x[1 : planes - 1] for x in pieces] if planes > 2 else []

    def across_y(items):
        return [
            lax.ppermute(x, "py", [(i, i ^ k) for i in range(parts)]) if k else x
            for k, x in enumerate(items)
        ]

    edges = across_y(edges)
    inner = across_y(inner)
    drive = (
        excite_gain * potential * (potential - threshold) * (1.0 - potential) - potential * recovery
    )
    v_star = potential + time_step * (drive + stimulus)
    rate = base_rate + rate_slope * recovery / (potential + rate_shift)
    recovery_next = recovery + time_step * rate * (
        -recovery - excite_gain * potential * (potential - threshold - 1.0)
    )
    ulo, uhi = neighbours(v_star[:1], v_star[-1:], AXES)

    slab = (planes, gy, gz)
    payload = (sh.chips, sh.rows + SUB, LANE)
    carries = (sh.chips, sh.rows, LANE)
    sums = (sh.tiles + 1, SUB, LANE)
    parted = (sh.tiles, SUB, LANE)
    swap = [(i, i ^ 1) for i in range(devices)]
    same_core = [[2 * chip + side for chip in range(sh.chips)] for side in range(2)]
    plane = (1, gy, gz)
    first, last = call(
        functools.partial(edge_kernel, sh, parts), "edges", [plane, plane], [place] + edges
    )
    clo, chi = neighbours(first, last, AXES)
    gxf, gyf, gzf, r, f = call(
        functools.partial(start_kernel, sh, parts),
        "start",
        [(planes + 1, gy, gz), slab, slab, slab, slab],
        [place, v_star, first, last] + inner + [tables],
        [pltpu.VMEM(slab, jnp.float32)],
    )
    operands = [core, v_star, ulo, uhi, clo, chi, first, last, rho, tables, gxf, r, f]
    gxf, r, f, keep, send = call(
        functools.partial(border_kernel, sh),
        "border",
        [(planes + 1, gy, gz), slab, slab, sums, sums],
        operands,
        aliases={10: 0, 11: 1, 12: 2},
    )
    spectral = [
        pltpu.VMEM((planes + 2, gy, gz), jnp.bfloat16),
        pltpu.VMEM((planes + 2, gy, gz), jnp.bfloat16),
        pltpu.VMEM((planes + 2, gy, gz), jnp.float32),
    ]
    coefs = []
    basis = []
    z = w = s = q = t = None
    for stage in range(ITERS):
        other = lax.ppermute(send, AXES, swap)
        (pay,) = call(
            functools.partial(join_kernel, sh, stage > 0),
            f"join{stage}",
            [payload if stage > 0 else carries],
            [core, keep, other, across],
        )
        recv = exchange(pay, same_core)
        if stage == 0:
            (carry,) = call(
                functools.partial(scan_kernel, sh, True),
                "scan0",
                [carries],
                [recv, block, closure, onward],
            )
        else:
            carry, coef = call(
                functools.partial(scan_kernel, sh, False),
                f"scan{stage}",
                [carries, (SUB, gz)],
                [recv, block, closure, onward, coef],
            )
            coefs.append(coef)
        carry = exchange(carry, same_core)
        own, send = call(
            functools.partial(part_kernel, sh),
            f"part{stage}",
            [parted, parted],
            [core, carry, keep, other, across],
        )
        if stage == ITERS - 1:
            send, now = lax.optimization_barrier((send, coef))
            before, direction = call(
                functools.partial(blend_kernel, sh),
                "blend",
                [slab, slab],
                coefs[:-1] + [now, v_star] + basis,
            )
        other = lax.ppermute(send, AXES, swap)
        if stage == ITERS - 1:
            other, before, direction = lax.optimization_barrier((other, before, direction))
        operands = [core, f, own, other, rho, scale, tables, gxf, gyf, gzf, r]
        if stage > 0:
            operands += [coef, z, w]
        if stage > 1:
            operands += [s, q, t]
        kernel = functools.partial(step_kernel, sh, stage)
        if stage == 0:
            shapes = [slab, slab, slab, sums, sums]
            z, w, f, keep, send = call(kernel, "step0", shapes, operands, spectral)
        elif stage < ITERS - 1:
            shapes = [slab] * (5 if stage == 1 else 6) + [slab, sums, sums]
            old_w = w
            results = call(kernel, f"step{stage}", shapes, operands, spectral)
            if stage == 1:
                z, w, r, q, t, f, keep, send = results
                s = old_w
            else:
                z, w, r, s, q, t, f, keep, send = results
        else:
            z, pay = call(kernel, f"step{stage}", [slab, (devices, 1, LANE)], operands, spectral)
        basis.append(z)
    recv = exchange(pay)
    (potential_next,) = call(
        functools.partial(finish_kernel, sh),
        "finish",
        [slab],
        [coef, recv, before, direction, z],
        [pltpu.VMEM(slab, jnp.float32), pltpu.SemaphoreType.DMA((planes,))],
        out_space=pl.ANY,
    )
    return potential_next, recovery_next


def solution(mesh):
    in_specs = (
        P(AXES, None, None),
        P(AXES, None, None),
        P(AXES, None, None),
        P("px", "py", None),
    )
    out_specs = (P(AXES, None, None), P(AXES, None, None))
    return jax.shard_map(local, mesh=mesh, in_specs=in_specs, out_specs=out_specs, check_vma=False)
```
